128 devices in a mesh: psr: 16 (over x, z), toa: 8 (over y, core).
Axes of the slice: x: 4, y: 4, z: 4, core: 2. Of those that a mesh axis runs over, the one named last changes fastest.
Arguments:
- design: bfloat16 [12288, 128, 256], P(('psr', 'toa')), may hold values from -0.035888672 to 0.035888672
- noise_weight: float32 [12288, 128], P(('psr', 'toa')), may hold values from 0.3 to 3
- residuals: bfloat16 [12288, 128], P(('psr', 'toa')), may hold values from -6 to 6
- slot_pulsar: int32 [12288], P(('psr', 'toa')), may hold values from 0 to 7, as said below
- slot_rows: int32 [12288], P(('psr', 'toa')), may hold values from 0 to 128, as said below
- own_prior: float32 [128, 192], P(('psr', 'toa')), may hold values from 0.2 to 5
- spectrum: float32 [32], replicated, may hold values from 0.05 to 2
- directions: float32 [3, 128], replicated, may hold values from -1 to 1, as said below
Outputs:
- coeffs: float32 [128, 64], P(('psr', 'toa'))
- log_dets: float32 [128], P(('psr', 'toa'))
- chi_square: float32 [128], P(('psr', 'toa'))
The draws below stay inside these ranges and needn't reach their ends.
Inputs may be any that keep to these rules, and one draw needn't show every extreme that they name: `slot_pulsar`: pulsar k of group g is pulsar g * 8 + k of the arrays with a pulsar dimension; empty blocks name pulsar 0. `slot_rows`: on each device the blocks holding TOAs come first and the empty ones (0 rows) last; within a psr group a pulsar's blocks are consecutive in device order, cyclically, all full but its last; every pulsar has between 8 * 96 * 4 and 8 * 96 * 16 TOAs. `directions`: unit vectors; any two are at least 0.1 radians apart.
All inputs are finite; a program needn't handle non-finite values.
Results may differ from the reference program's by a relative error of at most 0.003.
Values sent between devices are 32-bit elements; how exact they have to be, the bound alone decides.
No kernel may reach another device: no remote copies, remote signals or barrier semaphores. Data moves between devices by JAX's collectives and lax.ppermute only.
A program may use at most 128 MiB of HBM per device.

```python
import math
import jax
import jax.numpy as jnp
from jax import lax

GROUP_PULSARS = 8
PULSARS = 128
COLUMNS = 256
FREQS = 32
OWN = 192
BLOCK_ROWS = 128
SLOTS = 96
BLOCKS = 12288
ITERS = 8
N_PSR = 16
N_TOA = 8


def slot_layout(key):
    capacity = N_TOA * SLOTS
    pulsar_cap = capacity * BLOCK_ROWS // GROUP_PULSARS
    toa_counts = jax.random.randint(jax.random.fold_in(key, 101), (N_PSR, GROUP_PULSARS), pulsar_cap // 4, pulsar_cap + 1)
    blocks = (toa_counts + BLOCK_ROWS - 1) // BLOCK_ROWS
    block_ends = jnp.cumsum(blocks, axis=1)
    begins = block_ends - blocks
    first_device = jax.random.randint(jax.random.fold_in(key, 102), (N_PSR, 1), 0, N_TOA)
    position = jnp.arange(capacity, dtype=jnp.int32)[None, :]
    group_block = (position - first_device * SLOTS) % capacity
    inside = (group_block[:, :, None] >= begins[:, None, :]) & (group_block[:, :, None] < block_ends[:, None, :])
    serial = jnp.arange(GROUP_PULSARS, dtype=jnp.int32)[None, None, :]
    pulsar = jnp.sum(jnp.where(inside, serial, 0), axis=2)
    filled = jnp.any(inside, axis=2)
    last_block = jnp.sum(jnp.where(inside, (block_ends - 1)[:, None, :], 0), axis=2)
    tail_rows = jnp.sum(jnp.where(inside, (toa_counts - BLOCK_ROWS * (blocks - 1))[:, None, :], 0), axis=2)
    row_count = jnp.where(filled, jnp.where(group_block == last_block, tail_rows, BLOCK_ROWS), 0)
    return (pulsar.reshape(-1).astype(jnp.int32), row_count.reshape(-1).astype(jnp.int32))


def draw_slot_pulsar(key, part):
    return slot_layout(key)[0]


def draw_slot_rows(key, part):
    return slot_layout(key)[1]


def draw_directions(key, part):
    clusters = N_PSR
    members = GROUP_PULSARS
    number = clusters * members
    serial = jnp.arange(clusters).astype(jnp.float32)
    offset_angle = jax.random.uniform(jax.random.fold_in(key, 201), (), jnp.float32, 0.0, 6.2831853)
    height = 1.0 - (2.0 * serial + 1.0) / clusters
    azimuth = 2.39996323 * serial + offset_angle
    radius = jnp.sqrt(jnp.maximum(1.0 - height * height, 0.0))
    centre = jnp.stack([radius * jnp.cos(azimuth), radius * jnp.sin(azimuth), height], axis=1)
    east_axis = jnp.stack([-jnp.sin(azimuth), jnp.cos(azimuth), jnp.zeros_like(azimuth)], axis=1)
    north_axis = jnp.cross(centre, east_axis)
    cycle_size = jax.random.uniform(jax.random.fold_in(key, 202), (clusters, 1), jnp.float32, 0.135, 0.16)
    cycle_turn = jax.random.uniform(jax.random.fold_in(key, 203), (clusters, 1), jnp.float32, 0.0, 6.2831853)
    spoke_shake = jax.random.uniform(jax.random.fold_in(key, 204), (clusters, members), jnp.float32, -0.03, 0.03)
    radial_shake = jax.random.uniform(jax.random.fold_in(key, 205), (clusters, members), jnp.float32, 0.97, 1.03)
    member_index = jnp.arange(members).astype(jnp.float32)[None, :]
    spoke_angle = 6.2831853 * (member_index - 1.0) / (members - 1) + cycle_turn + spoke_shake
    distance = jnp.where(member_index > 0.5, cycle_size * radial_shake, 0.0)
    across = jnp.cos(spoke_angle)[:, :, None] * east_axis[:, None, :] + jnp.sin(spoke_angle)[:, :, None] * north_axis[:, None, :]
    points = jnp.cos(distance)[:, :, None] * centre[:, None, :] + jnp.sin(distance)[:, :, None] * across
    points = points.reshape((number, 3)).T
    shuffle = jax.random.permutation(jax.random.fold_in(key, 206), number)
    return points[:, shuffle].astype(jnp.float32)


def levels(rng, extent, split, smallest, largest):
    factor_of, own = 1.0, jax.random.fold_in(rng, 6)
    for axis_at, parts in split:
        draws = jnp.exp(jax.random.uniform(jax.random.fold_in(own, axis_at), (parts,), jnp.float32, smallest / len(split), largest / len(split)))
        factor_of = factor_of * jnp.repeat(draws, extent[axis_at] // parts).reshape([-1 if axis == axis_at else 1 for axis in range(len(extent))])
    return factor_of


def bell_draw(stream_key, dims, deviation, bound, cuts=(), held_as=jnp.bfloat16):
    level = levels(stream_key, dims, cuts, -0.22, 0.18) if cuts else 1.0
    array = jax.random.normal(stream_key, dims, jnp.float32) * deviation * level
    return jnp.minimum(jnp.maximum(array, -bound), bound).astype(held_as)


def setup_inputs(seed: int = 0) -> dict:
    keys = jax.random.split(jax.random.key(seed), 9)
    return {
        "design": bell_draw(keys[0], (BLOCKS, BLOCK_ROWS, COLUMNS), 0.006, 0.035888672, ((0, 128),)),
        "noise_weight": jnp.clip(jnp.exp(math.log(3.0) - 2.3025851 * jax.random.uniform(keys[1], (BLOCKS, BLOCK_ROWS), jnp.float32) ** levels(keys[1], (BLOCKS, BLOCK_ROWS), ((0, 128),), -0.2, 0.2)), 0.3, 3.0),
        "residuals": bell_draw(keys[2], (BLOCKS, BLOCK_ROWS), 1.0, 6.0, ((0, 128),)),
        "slot_pulsar": draw_slot_pulsar(jax.random.fold_in(keys[8], 71), 0),
        "slot_rows": draw_slot_rows(jax.random.fold_in(keys[8], 71), 0),
        "own_prior": jnp.clip(jnp.exp(math.log(5.0) - 3.218876 * jax.random.uniform(keys[5], (PULSARS, OWN), jnp.float32) ** levels(keys[5], (PULSARS, OWN), ((0, 128),), -0.2, 0.2)), 0.2, 5.0),
        "spectrum": jnp.clip(jnp.exp(jax.random.uniform(keys[6], (FREQS,), jnp.float32, math.log(0.05), math.log(2.0))), 0.05, 2.0),
        "directions": draw_directions(jax.random.fold_in(keys[8], 71), 0),
    }


highest = lax.Precision.HIGHEST

def cholesky_solve(factor, right_side):
    halfway = lax.linalg.triangular_solve(factor, right_side, left_side=True, lower=True)
    return lax.linalg.triangular_solve(factor, halfway, left_side=True, lower=True, transpose_a=True)

def slot_term_values(design, weight, residuals, pulsar, slot_rows):
    positions = lax.broadcasted_iota(jnp.int32, weight.shape, 1)
    weight = jnp.where(positions < slot_rows[:, None], weight, 0.0)
    weighted = (weight[:, :, None] * design.astype(jnp.float32)).astype(jnp.bfloat16)
    weighted = lax.optimization_barrier(weighted)
    wide_weighted = weighted.astype(jnp.float32)
    wide_design = design.astype(jnp.float32)
    wide_residual = residuals.astype(jnp.float32)
    products = jnp.einsum('srk,srl->skl', wide_weighted, wide_design, precision=highest)
    fitted = jnp.einsum('srk,sr->sk', wide_weighted, wide_residual, precision=highest)
    energy = jnp.sum(weight * wide_residual * wide_residual, axis=1)
    owners = (pulsar[:, None] == lax.broadcasted_iota(jnp.int32, (pulsar.shape[0], GROUP_PULSARS), 1)).astype(jnp.float32)
    return (jnp.einsum('sp,skl->pkl', owners, products, precision=highest), jnp.einsum('sp,sk->pk', owners, fitted, precision=highest), jnp.dot(energy, owners, precision=highest), jnp.dot(slot_rows.astype(jnp.float32), owners, precision=highest))

def group_grams(design, weight, residuals, pulsar, slot_rows):
    count_blocks = design.shape[0] // 16
    column_count = design.shape[2]

    def regroup(member):
        return member.reshape((count_blocks, 16) + member.shape[1:])

    def one_block(running_total, group_members):
        summand_terms = slot_term_values(*group_members)
        return (tuple((earlier_term + later_term for earlier_term, later_term in zip(running_total, summand_terms))), 0)
    initial = (jnp.zeros((GROUP_PULSARS, column_count, column_count), jnp.float32), jnp.zeros((GROUP_PULSARS, column_count), jnp.float32), jnp.zeros((GROUP_PULSARS,), jnp.float32), jnp.zeros((GROUP_PULSARS,), jnp.float32))
    group_members = tuple((regroup(member) for member in (design, weight, residuals, pulsar, slot_rows)))
    totals, unused = lax.scan(one_block, initial, group_members)
    return totals

def eliminate(gram_sums, projections, own_prior):
    column_count = gram_sums.shape[1]
    common = column_count - own_prior.shape[1]
    identity = jnp.eye(own_prior.shape[1], dtype=jnp.float32)
    own_block = gram_sums[:, common:, common:] + (1.0 / own_prior)[:, :, None] * identity[None, :, :]
    factor = jnp.linalg.cholesky(own_block)
    right_side = jnp.concatenate([gram_sums[:, common:, :common], projections[:, common:, None]], axis=2)
    solved = cholesky_solve(factor, right_side)
    cross_block = gram_sums[:, :common, common:]
    reduced = jnp.einsum('pck,pkd->pcd', cross_block, solved, precision=highest)
    schur_part = gram_sums[:, :common, :common] - reduced[:, :, :common]
    target = projections[:, :common] - reduced[:, :, common]
    quadratic = jnp.sum(projections[:, common:] * solved[:, :, common], axis=1)
    own_logdet = 2.0 * jnp.sum(jnp.log(jnp.diagonal(factor, axis1=1, axis2=2)), axis=1)
    return (schur_part, target, quadratic, own_logdet)

def coupling_inverse(directions):
    cosines = jnp.clip(jnp.dot(directions.T, directions, precision=highest), -1.0, 1.0)
    number = cosines.shape[0]
    diagonal = jnp.eye(number, dtype=jnp.float32) > 0.5
    spread = jnp.where(diagonal, 1.0, 0.5 * (1.0 - cosines))
    intersect_curve = 1.5 * spread * jnp.log(spread) - 0.25 * spread + 0.5
    correlation = jnp.where(diagonal, 1.0, intersect_curve)
    factor = jnp.linalg.cholesky(correlation)
    return cholesky_solve(factor, jnp.eye(number, dtype=jnp.float32))

def coupled_apply(schur_part, coupling, inverse_power, vector):
    within = jnp.einsum('pcd,pd->pc', schur_part, vector, precision=highest)
    mixing = jnp.dot(coupling, vector, precision=highest)
    return within + mixing * inverse_power[None, :]

def precondition(block_factor, residual):
    return cholesky_solve(block_factor, residual[:, :, None])[:, :, 0]

def reference(design, noise_weight, residuals, slot_pulsar, slot_rows, own_prior, spectrum, directions):
    groups = N_PSR
    group_slots = design.shape[0] // groups
    shaped = tuple((member.reshape((groups, group_slots) + member.shape[1:]) for member in (design, noise_weight, residuals, slot_pulsar, slot_rows)))

    def per_group(group_members):
        return group_grams(*group_members)
    gram_sums, projections, energy, counts = lax.map(per_group, shaped)
    gram_sums = gram_sums.reshape((PULSARS, COLUMNS, COLUMNS))
    projections = projections.reshape((PULSARS, COLUMNS))
    energy = energy.reshape((PULSARS,))
    counts = counts.reshape((PULSARS,))
    schur_part, target, quadratic, own_logdet = eliminate(gram_sums, projections, own_prior)
    coupling = coupling_inverse(directions)
    inverse_power = 1.0 / jnp.repeat(spectrum, 2)
    block_matrix = schur_part + jnp.diagonal(coupling)[:, None, None] * jnp.diag(inverse_power)[None, :, :]
    block_factor = jnp.linalg.cholesky(block_matrix)
    block_logdet = 2.0 * jnp.sum(jnp.log(jnp.diagonal(block_factor, axis1=1, axis2=2)), axis=1)
    solution = jnp.zeros_like(target)
    residual = target
    scaled = precondition(block_factor, residual)
    direction = scaled
    inner_now = jnp.sum(residual * scaled)
    for iteration in range(ITERS):
        mapped = coupled_apply(schur_part, coupling, inverse_power, direction)
        step_size = inner_now / jnp.sum(direction * mapped)
        solution = solution + step_size * direction
        residual = residual - step_size * mapped
        if iteration + 1 < ITERS:
            scaled = precondition(block_factor, residual)
            inner_next = jnp.sum(residual * scaled)
            direction = scaled + inner_next / inner_now * direction
            inner_now = inner_next
    log_dets = (own_logdet + block_logdet) / COLUMNS
    chi_square = (energy - quadratic - jnp.sum(target * solution, axis=1)) / counts
    return (solution, log_dets, chi_square)
```

```python
import jax
import jax.numpy as jnp
from jax import lax
from jax.experimental import pallas as pl
from jax.experimental.pallas import tpu as pltpu
from jax.sharding import PartitionSpec as P

GROUP_PULSARS = 8
ITERS = 8
COLUMNS = 256
COMMON = 64
STEP_BLOCKS = 16
ROWS_SENT = 264
WIDTH = 2176
AXES = ("psr", "toa")

highest = lax.Precision.HIGHEST
f32 = jnp.float32


def iota(shape, dim):
    return lax.broadcasted_iota(jnp.int32, shape, dim)


def sub_bcast(value, row):
    return jnp.broadcast_to(value[row : row + 1, :], value.shape)


def lane_bcast(value, lane):
    return jnp.broadcast_to(value[:, lane : lane + 1], value.shape)


def total(value):
    return jnp.sum(jnp.sum(value, axis=0, keepdims=True), axis=1, keepdims=True)


def eliminate_rows(tiles, first_lane, log_sum):
    count = len(tiles)
    width = len(tiles[0])
    row = iota((8, 128), 0)
    for b in range(count):
        at = first_lane + 8 * b
        tile, lane = at // 128, at % 128
        cols = [lane_bcast(tiles[b][tile], lane + k) for k in range(8)]
        for i in range(8):
            here = row == i
            pivot = sub_bcast(cols[i], i)
            inverse = 1.0 / pivot
            log_sum = log_sum + jnp.log(pivot)
            column = cols[i]
            for k in range(8):
                if k != i:
                    scaled = sub_bcast(cols[k], i) * inverse
                    cols[k] = jnp.where(here, scaled, cols[k] - column * scaled)
            cols[i] = jnp.where(here, inverse, -column * inverse)
        fresh = []
        for t in range(width):
            parts = [cols[k] * sub_bcast(tiles[b][t], k) for k in range(8)]
            while len(parts) > 1:
                parts = [u + v for u, v in zip(parts[::2], parts[1::2])]
            fresh.append(parts[0])
        spread = [[sub_bcast(fresh[t], k) for k in range(8)] for t in range(width)]
        for a in range(count):
            if a != b:
                factor = [lane_bcast(tiles[a][tile], lane + k) for k in range(8)]
                for t in range(width):
                    value = tiles[a][t]
                    for k in range(8):
                        value = value - factor[k] * spread[t][k]
                    tiles[a][t] = value
        tiles[b] = fresh
    return tiles, log_sum


def gram_kernel(
    pulsar_ref,
    rows_ref,
    place_ref,
    design_ref,
    weight_ref,
    resid_ref,
    mine_ref,
    other_ref,
    gram,
    fit,
    energy,
    wide_resid,
    counts,
):
    step = pl.program_id(0)

    @pl.when(step == 0)
    def _():
        gram[...] = jnp.zeros(gram.shape, f32)
        fit[...] = jnp.zeros(fit.shape, f32)
        energy[...] = jnp.zeros(energy.shape, f32)
        for k in range(GROUP_PULSARS):
            counts[k] = 0

    wide_resid[...] = resid_ref[...].astype(f32)
    lane = iota((1, 128), 1)

    def add_blocks(local, number, pulsar):
        pieces, fitted, squares = [], None, None
        for i in range(number):
            valid = rows_ref[step * STEP_BLOCKS + local + i]
            weight = jnp.where(lane < valid, weight_ref[pl.ds(local + i, 1), :], 0.0)
            resid = wide_resid[pl.ds(local + i, 1), :]
            turned = design_ref[local + i].T.astype(f32)
            weighted = (turned * weight).astype(jnp.bfloat16)
            pieces.append(weighted)
            product = weighted.astype(f32) * resid
            square = weight * resid * resid
            fitted = product if fitted is None else fitted + product
            squares = square if squares is None else squares + square
            counts[pulsar] = counts[pulsar] + valid
        left = jnp.concatenate(pieces, axis=1) if number > 1 else pieces[0]
        right = design_ref[pl.ds(local, number)].reshape(number * 128, COLUMNS)
        gram[pulsar] = gram[pulsar] + jnp.dot(left, right, preferred_element_type=f32)
        fit[pulsar] = fit[pulsar] + fitted
        energy[pl.ds(pulsar, 1), :] = energy[pl.ds(pulsar, 1), :] + squares

    def quad(q, carry):
        at = step * STEP_BLOCKS + q * 4
        pulsars = [pulsar_ref[at + i] for i in range(4)]
        filled = rows_ref[at] + rows_ref[at + 1] + rows_ref[at + 2] + rows_ref[at + 3] > 0
        same = (
            (pulsars[0] == pulsars[1])
            & (pulsars[1] == pulsars[2])
            & (pulsars[2] == pulsars[3])
        )

        @pl.when(filled & same)
        def _():
            add_blocks(q * 4, 4, pulsars[0])

        @pl.when(filled & jnp.logical_not(same))
        def _():
            for i in range(4):
                add_blocks(q * 4 + i, 1, pulsars[i])

        return carry

    lax.fori_loop(0, STEP_BLOCKS // 4, quad, 0)

    @pl.when(step == pl.num_programs(0) - 1)
    def _():
        row, col = iota((128, 128), 0), iota((128, 128), 1)
        line = iota((8, 128), 0)
        spot = iota((8, 128), 1)

        def pack(out_ref, s, k):
            @pl.when(counts[k] == 0)
            def _():
                out_ref[s] = jnp.zeros((ROWS_SENT, 128), f32)

            @pl.when(counts[k] > 0)
            def _():
                upper = gram[k, 0:128, 0:128]
                lower = gram[k, 128:256, 128:256]
                upper = 0.5 * (upper + upper.T)
                lower = 0.5 * (lower + lower.T)
                cross = 0.5 * (gram[k, 128:256, 0:128] + gram[k, 0:128, 128:256].T)
                out_ref[s, 0:128, :] = jnp.where(col > row, upper, lower)
                out_ref[s, 128:256, :] = cross
                diagonal = jnp.sum(jnp.where(col == row, upper, 0.0), axis=0, keepdims=True)
                first = jnp.sum(fit[k, 0:128, :].T, axis=0, keepdims=True)
                second = jnp.sum(fit[k, 128:256, :].T, axis=0, keepdims=True)
                power = jnp.sum(energy[pl.ds(k, 1), :], axis=1, keepdims=True)
                number = counts[k].astype(f32)
                last = jnp.where(spot == 0, power, jnp.where(spot == 1, number, 0.0))
                rest = jnp.where(line == 3, last, 0.0)
                rest = jnp.where(line == 0, diagonal, rest)
                rest = jnp.where(line == 1, first, rest)
                out_ref[s, 256:264, :] = jnp.where(line == 2, second, rest)

        height = place_ref[0]
        core = place_ref[1]
        for s in range(4):
            base = 2 * ((height + s) & 3)
            pack(mine_ref, s, base + core)
            pack(other_ref, s, base + 1 - core)


def gram_parts(place, design, weight, residuals, slot_pulsar, slot_rows):
    slots = design.shape[0]
    piece = jax.ShapeDtypeStruct((4, ROWS_SENT, 128), f32)
    whole = pl.BlockSpec((4, ROWS_SENT, 128), lambda i, *_: (0, 0, 0))
    return pl.pallas_call(
        gram_kernel,
        grid_spec=pltpu.PrefetchScalarGridSpec(
            num_scalar_prefetch=3,
            grid=(slots // STEP_BLOCKS,),
            in_specs=[
                pl.BlockSpec((STEP_BLOCKS, 128, COLUMNS), lambda i, *_: (i, 0, 0)),
                pl.BlockSpec((STEP_BLOCKS, 128), lambda i, *_: (i, 0)),
                pl.BlockSpec((STEP_BLOCKS, 128), lambda i, *_: (i, 0)),
            ],
            out_specs=[whole, whole],
            scratch_shapes=[
                pltpu.VMEM((GROUP_PULSARS, COLUMNS, COLUMNS), f32),
                pltpu.VMEM((GROUP_PULSARS, COLUMNS, 128), f32),
                pltpu.VMEM((GROUP_PULSARS, 128), f32),
                pltpu.VMEM((STEP_BLOCKS, 128), f32),
                pltpu.SMEM((GROUP_PULSARS,), jnp.int32),
            ],
        ),
        out_shape=[piece, piece],
        name="gram",
    )(slot_pulsar, slot_rows, place, design, weight, residuals)


def coupling_kernel(place_ref, directions_ref, out_ref):
    core = place_ref[1]
    row, col = iota((128, 128), 0), iota((128, 128), 1)
    source = jnp.where(col < 64, 2 * col + core, 2 * col - 127 - core)
    chosen = (row == source).astype(f32)
    lines = jnp.concatenate([directions_ref[...], jnp.zeros((5, 128), f32)], axis=0)
    lines = jnp.dot(lines, chosen, precision=highest, preferred_element_type=f32)
    turned = lines.T
    cosines = jnp.zeros((128, 128), f32)
    for i in range(3):
        cosines = cosines + turned[:, i : i + 1] * lines[i : i + 1, :]
    cosines = jnp.clip(cosines, -1.0, 1.0)
    same = row == col
    spread = jnp.where(same, 1.0, 0.5 * (1.0 - cosines))
    curve = 1.5 * spread * jnp.log(spread) - 0.25 * spread + 0.5
    correlation = jnp.where(same, 1.0, curve)
    identity = jnp.where(same, 1.0, 0.0)
    tiles = [
        [correlation[8 * a : 8 * a + 8, :], identity[8 * a : 8 * a + 8, :]] for a in range(16)
    ]
    tiles, _ = eliminate_rows(tiles, 0, jnp.zeros((8, 128), f32))
    for a in range(16):
        out_ref[8 * a : 8 * a + 8, :] = tiles[a][1]


def coupling_inverse(place, directions):
    return pl.pallas_call(
        coupling_kernel,
        in_specs=[
            pl.BlockSpec(memory_space=pltpu.SMEM),
            pl.BlockSpec(memory_space=pltpu.VMEM),
        ],
        out_specs=pl.BlockSpec(memory_space=pltpu.VMEM),
        out_shape=jax.ShapeDtypeStruct((128, 128), f32),
        name="coupling",
    )(place, directions)


def power_column(spectrum_ref):
    inverse = 1.0 / spectrum_ref[...]
    half = iota((64, 32), 0) >> 1
    spread = jnp.where(iota((64, 32), 1) == half, jnp.broadcast_to(inverse, (64, 32)), 0.0)
    return jnp.sum(spread, axis=1, keepdims=True)


def own_kernel(
    place_ref,
    part0,
    part1,
    part2,
    part3,
    prior_ref,
    spectrum_ref,
    coupling_ref,
    sent_ref,
    extra_ref,
    logdet_ref,
    work,
):
    row, col = iota((128, 128), 0), iota((128, 128), 1)

    def summed(lo, hi):
        return (part0[lo:hi, :] + part1[lo:hi, :]) + (part2[lo:hi, :] + part3[lo:hi, :])

    packed = summed(0, 128)
    cross = summed(128, 256)
    rest = summed(256, 264)
    turned = packed.T
    prior = 1.0 / prior_ref[...]
    prior = jnp.concatenate([jnp.zeros((1, 64), f32), prior], axis=1)
    upper = jnp.where(col > row, packed, turned)
    upper = jnp.where(col == row, rest[0:1, :] + prior[:, 0:128], upper)
    lower = jnp.where(col <= row, packed, turned)
    lower = jnp.where(col == row, lower + prior[:, 128:256], lower)
    work[0:128, 0:128] = upper
    work[128:256, 128:256] = lower
    work[128:256, 0:128] = cross
    work[0:128, 128:256] = cross.T
    side = rest.T
    work[0:128, 256:384] = jnp.broadcast_to(side[:, 1:2], (128, 128))
    work[128:256, 256:384] = jnp.broadcast_to(side[:, 2:3], (128, 128))

    log_sum = jnp.zeros((8, 128), f32)
    quadratic = jnp.zeros((64, 128), f32)
    for panel in range(3):
        at = COMMON + 64 * panel
        old = work[at : at + 64, :]
        tiles = [
            [old[8 * a : 8 * a + 8, 128 * t : 128 * t + 128] for t in range(3)] for a in range(8)
        ]
        tiles, log_sum = eliminate_rows(tiles, at, log_sum)
        fresh = [jnp.concatenate([tiles[a][t] for a in range(8)], axis=0) for t in range(3)]
        quadratic = quadratic + old[:, 256:384] * fresh[2]
        final = panel == 2
        for t in (0,) if final else (0, 1):
            left = old[:, 128 * t : 128 * t + 128]
            for u in (0, 2) if final else (0, 1, 2):
                change = lax.dot_general(
                    left,
                    fresh[u],
                    (((0,), (0,)), ((), ())),
                    precision=highest,
                    preferred_element_type=f32,
                )
                where = (slice(128 * t, 128 * t + 128), slice(128 * u, 128 * u + 128))
                work[where] = work[where] - change

    own = place_ref[2]
    mine = jnp.where((row == own) & (col == own), coupling_ref[...], 0.0)
    self_coupling = total(mine)
    power = power_column(spectrum_ref)
    row64, col64 = iota((64, 128), 0), iota((64, 128), 1)
    block = work[0:64, 0:128]
    block = jnp.where(row64 == col64, block + self_coupling * power, block)
    block = jnp.where(col64 < 64, block, jnp.where(col64 == row64 + 64, 1.0, 0.0))
    tiles = [[block[8 * a : 8 * a + 8, :]] for a in range(8)]
    tiles, log_sum = eliminate_rows(tiles, 0, log_sum)
    solved = jnp.concatenate([tiles[a][0] for a in range(8)], axis=0)
    inverse = pltpu.roll(solved, 64, 1)
    top, bottom = inverse[0:32, :], inverse[32:64, :]
    row32, col32 = iota((32, 128), 0), iota((32, 128), 1)
    moved = pltpu.roll(bottom, 96, 1)
    triangle = jnp.where(col32 > row32, top, moved)
    folded = jnp.where(col32 < 32, triangle, top)
    lines = jnp.where(
        iota((16, 128), 1) < 64, folded[0:16, :], pltpu.roll(folded[16:32, :], 64, 1)
    )
    diagonal = jnp.sum(jnp.where(row32 == col32, top, 0.0), axis=0, keepdims=True)
    target = work[0:64, 256:384]
    target_line = jnp.concatenate([target, target], axis=0).T[0:1, :]
    final_line = jnp.where(iota((1, 128), 1) < 64, diagonal, target_line)
    for i in range(16):
        sent_ref[:, 128 * i : 128 * i + 128] = jnp.broadcast_to(lines[i : i + 1, :], (64, 128))
    sent_ref[:, 2048:2176] = jnp.broadcast_to(final_line, (64, 128))
    spent = jnp.sum(quadratic, axis=0, keepdims=True)
    left_over = rest[3:4, 0:1] - spent[:, 0:1]
    line = iota((8, 128), 0)
    extra_ref[...] = jnp.where(line == 0, left_over, rest[3:4, 1:2])
    logdet_ref[0] = log_sum[0, 0] / COLUMNS


def own_terms(place, parts, own_prior, spectrum, coupling):
    vmem = pl.BlockSpec(memory_space=pltpu.VMEM)
    smem = pl.BlockSpec(memory_space=pltpu.SMEM)
    return pl.pallas_call(
        own_kernel,
        in_specs=[smem] + [vmem] * 7,
        out_specs=[vmem, vmem, smem],
        out_shape=[
            jax.ShapeDtypeStruct((64, WIDTH), f32),
            jax.ShapeDtypeStruct((8, 128), f32),
            jax.ShapeDtypeStruct((1,), f32),
        ],
        scratch_shapes=[pltpu.VMEM((COLUMNS, 384), f32)],
        name="own",
    )(place, *parts, own_prior, spectrum, coupling)


def gradient_kernel(
    place_ref,
    near_ref,
    far_ref,
    coupling_ref,
    spectrum_ref,
    extra_ref,
    coeffs_ref,
    chi_ref,
    flat,
    inverse,
    resid,
    direction,
    mapped,
    answer,
    turned,
):
    for i in range(WIDTH // 128):
        where = slice(128 * i, 128 * i + 128)
        flat[where, :] = jnp.concatenate([near_ref[:, where], far_ref[:, where]], axis=0).T
    line = iota((8, 128), 0)

    def start(r):
        return (r % 16) * 128 + (r // 16) * 64

    def across(c, offset):
        return flat[pl.ds(start(c) + offset, 8, stride=128), :]

    for r in range(32):
        at = start(r)
        corner = flat[2048 + r : 2049 + r, :]
        for c in range(0, 32, 8):
            straight = None if c + 7 < r else flat[at + c : at + c + 8, :]
            crossed = None if c > r else across(c, r)
            if straight is None:
                first = second = crossed
                second = None
            if crossed is None:
                first = straight
            if straight is not None and crossed is not None:
                index = line + c
                first = jnp.where(index > r, straight, crossed)
                first = jnp.where(index == r, corner, first)
            inverse[r, c : c + 8, :] = first
            low = None if c > r else flat[at + c : at + c + 8, :]
            high = None if c + 7 <= r else across(c, r)
            if low is None:
                value = high
            elif high is None:
                value = low
            else:
                value = jnp.where(line + c <= r, low, high)
            inverse[32 + r, 32 + c : 40 + c, :] = value
            inverse[r, 32 + c : 40 + c, :] = flat[at + 32 + c : at + 40 + c, :]
            inverse[32 + r, c : c + 8, :] = across(c, 32 + r)

    row, col = iota((128, 128), 0), iota((128, 128), 1)
    mixing = jnp.where(row == col, 0.0, coupling_ref[...])
    power = power_column(spectrum_ref)
    resid[...] = flat[2112:2176, :]
    direction[...] = jnp.zeros((64, 128), f32)
    mapped[...] = jnp.zeros((64, 128), f32)
    answer[...] = jnp.zeros((64, 128), f32)

    def iterate(_, carry):
        inner, curved = carry
        now = resid[...]
        scaled = jnp.zeros((64, 128), f32)
        for k in range(64):
            scaled = scaled + inverse[k] * resid[k : k + 1, :]
        mixed = jnp.dot(scaled, mixing, precision=highest, preferred_element_type=f32)
        image = now + power * mixed
        old_mapped = mapped[...]
        inner_next = total(now * scaled)
        straight = total(scaled * image)
        crossing = total(scaled * old_mapped)
        ratio = inner_next / inner
        curved = straight + ratio * (2.0 * crossing + ratio * curved)
        step = inner_next / curved
        toward = scaled + ratio * direction[...]
        image = image + ratio * old_mapped
        direction[...] = toward
        mapped[...] = image
        answer[...] = answer[...] + step * toward
        resid[...] = now - step * image
        return inner_next, curved

    lax.fori_loop(0, ITERS, iterate, (jnp.ones((1, 1), f32), jnp.zeros((1, 1), f32)))
    own = place_ref[2]
    value = answer[...]
    gained = jnp.sum(flat[2112:2176, :] * value, axis=0, keepdims=True)
    lane = iota((1, 128), 1)
    gained = jnp.sum(jnp.where(lane == own, gained, 0.0), axis=1, keepdims=True)
    chi = (extra_ref[0:1, 0:1] - gained) / extra_ref[1:2, 0:1]
    chi_ref[0] = chi[0, 0]
    turned[...] = jnp.concatenate([value, value], axis=0).T
    coeffs_ref[...] = turned[pl.ds(own, 1), :][:, 0:64]


def conjugate(place, near, far, coupling, spectrum, extra):
    vmem = pl.BlockSpec(memory_space=pltpu.VMEM)
    smem = pl.BlockSpec(memory_space=pltpu.SMEM)
    square = pltpu.VMEM((64, 128), f32)
    return pl.pallas_call(
        gradient_kernel,
        in_specs=[smem] + [vmem] * 5,
        out_specs=[vmem, smem],
        out_shape=[jax.ShapeDtypeStruct((1, COMMON), f32), jax.ShapeDtypeStruct((1,), f32)],
        scratch_shapes=[
            pltpu.VMEM((WIDTH, 128), f32),
            pltpu.VMEM((64, 64, 128), f32),
            square,
            square,
            square,
            square,
            pltpu.VMEM((128, 128), f32),
        ],
        name="gradient",
    )(place, near, far, coupling, spectrum, extra)


def body(design, noise_weight, residuals, slot_pulsar, slot_rows, own_prior, spectrum, directions):
    toa = lax.axis_index("toa")
    device = lax.axis_index("psr") * lax.axis_size("toa") + toa
    count = lax.axis_size("psr") * lax.axis_size("toa")
    core = toa % 2
    place = jnp.stack([toa // 2, core, device // 2]).astype(jnp.int32)
    spectrum = spectrum.reshape(1, -1)
    mine, other = gram_parts(place, design, noise_weight, residuals, slot_pulsar, slot_rows)
    got = lax.ppermute(other, "toa", [(u, u ^ 1) for u in range(8)])
    parts = [mine[s] + got[s] for s in range(4)]
    for s in range(1, 4):
        parts[s] = lax.ppermute(parts[s], "toa", [(u, (u + 2 * s) % 8) for u in range(8)])
    coupling = coupling_inverse(place, directions)
    sent, extra, log_dets = own_terms(place, parts, own_prior, spectrum, coupling)
    groups = [list(range(c, count, 2)) for c in range(2)]
    near = lax.all_to_all(sent, AXES, 0, 0, tiled=True, axis_index_groups=groups)
    far = lax.ppermute(near, "toa", [(u, u ^ 1) for u in range(8)])
    coeffs, chi_square = conjugate(place, near, far, coupling, spectrum, extra)
    return (coeffs, log_dets, chi_square)


def solution(mesh):
    return jax.shard_map(
        body,
        mesh=mesh,
        in_specs=(
            P(AXES, None, None),
            P(AXES, None),
            P(AXES, None),
            P(AXES),
            P(AXES),
            P(AXES, None),
            P(),
            P(),
        ),
        out_specs=(P(AXES, None), P(AXES), P(AXES)),
        check_vma=False,
    )
```

```python
import jax
import jax.numpy as jnp
from jax import lax
from jax.experimental import pallas as pl
from jax.experimental.pallas import tpu as pltpu
from jax.sharding import PartitionSpec as P

GROUP_PULSARS = 8
ITERS = 8
COLUMNS = 256
COMMON = 64
STEP_BLOCKS = 8
ROWS_SENT = 264
WIDTH = 2176
LINES = WIDTH // 128
AXES = ("psr", "toa")

highest = lax.Precision.HIGHEST
f32 = jnp.float32


def in_vmem(value):
    return pltpu.with_memory_space_constraint(value, pltpu.VMEM)


def iota(shape, dim):
    return lax.broadcasted_iota(jnp.int32, shape, dim)


def sub_bcast(value, row):
    return jnp.broadcast_to(value[row : row + 1, :], value.shape)


def lane_bcast(value, lane):
    return jnp.broadcast_to(value[:, lane : lane + 1], value.shape)


def total(value):
    return jnp.sum(jnp.sum(value, axis=0, keepdims=True), axis=1, keepdims=True)


def eliminate_rows(tiles, first_lane, log_sum):
    count = len(tiles)
    width = len(tiles[0])
    row = iota((8, 128), 0)
    for b in range(count):
        at = first_lane + 8 * b
        tile, lane = at // 128, at % 128
        cols = [lane_bcast(tiles[b][tile], lane + k) for k in range(8)]
        for i in range(8):
            here = row == i
            pivot = sub_bcast(cols[i], i)
            inverse = 1.0 / pivot
            log_sum = log_sum + jnp.log(pivot)
            column = cols[i]
            for k in range(8):
                if k != i:
                    scaled = sub_bcast(cols[k], i) * inverse
                    cols[k] = jnp.where(here, scaled, cols[k] - column * scaled)
            cols[i] = jnp.where(here, inverse, -column * inverse)
        fresh = []
        for t in range(width):
            parts = [cols[k] * sub_bcast(tiles[b][t], k) for k in range(8)]
            while len(parts) > 1:
                parts = [u + v for u, v in zip(parts[::2], parts[1::2])]
            fresh.append(parts[0])
        spread = [[sub_bcast(fresh[t], k) for k in range(8)] for t in range(width)]
        for a in range(count):
            if a != b:
                factor = [lane_bcast(tiles[a][tile], lane + k) for k in range(8)]
                for t in range(width):
                    value = tiles[a][t]
                    for k in range(8):
                        value = value - factor[k] * spread[t][k]
                    tiles[a][t] = value
        tiles[b] = fresh
    return tiles, log_sum


def gram_kernel(
    pulsar_ref,
    rows_ref,
    place_ref,
    design_ref,
    weight_ref,
    resid_ref,
    mine_ref,
    other_ref,
    blocks,
    gram,
    fit,
    energy,
    wide_resid,
    counts,
    arrived,
):
    slots = weight_ref.shape[0]
    steps = slots // STEP_BLOCKS

    def load(step):
        where = pl.ds(step * STEP_BLOCKS, STEP_BLOCKS)
        return pltpu.make_async_copy(design_ref.at[where], blocks.at[where], arrived.at[step])

    for step in range(steps):
        load(step).start()
    gram[...] = jnp.zeros(gram.shape, f32)
    fit[...] = jnp.zeros(fit.shape, f32)
    energy[...] = jnp.zeros(energy.shape, f32)
    for k in range(GROUP_PULSARS):
        counts[k] = 0
    wide_resid[...] = resid_ref[...].astype(f32)
    lane = iota((1, 128), 1)

    def one_step(step, carry):
        load(step).wait()
        at = step * STEP_BLOCKS
        pulsars = [pulsar_ref[at + i] for i in range(STEP_BLOCKS)]
        rows = [rows_ref[at + i] for i in range(STEP_BLOCKS)]
        same = pulsars[1] == pulsars[0]
        for i in range(2, STEP_BLOCKS):
            same = same & (pulsars[i] == pulsars[0])
        low = jnp.where(same, pulsars[0], 0)
        high = jnp.where(same, pulsars[0] + 1, GROUP_PULSARS)

        def one_pulsar(pulsar, carry):
            valid = [jnp.where(pulsars[i] == pulsar, rows[i], 0) for i in range(STEP_BLOCKS)]
            number = valid[0]
            for i in range(1, STEP_BLOCKS):
                number = number + valid[i]

            @pl.when(number > 0)
            def _():
                pieces, fitted, squares = [], None, None
                for i in range(STEP_BLOCKS):
                    weight = jnp.where(lane < valid[i], weight_ref[pl.ds(at + i, 1), :], 0.0)
                    resid = wide_resid[pl.ds(at + i, 1), :]
                    turned = blocks[at + i].T.astype(f32)
                    weighted = (turned * weight).astype(jnp.bfloat16)
                    pieces.append(weighted)
                    product = weighted.astype(f32) * resid
                    square = weight * resid * resid
                    fitted = product if fitted is None else fitted + product
                    squares = square if squares is None else squares + square
                left = jnp.concatenate(pieces, axis=1)
                right = blocks[pl.ds(at, STEP_BLOCKS)].reshape(STEP_BLOCKS * 128, COLUMNS)
                gram[pulsar] = gram[pulsar] + jnp.dot(left, right, preferred_element_type=f32)
                fit[pulsar] = fit[pulsar] + fitted
                energy[pl.ds(pulsar, 1), :] = energy[pl.ds(pulsar, 1), :] + squares
                counts[pulsar] = counts[pulsar] + number

            return carry

        return lax.fori_loop(low, high, one_pulsar, carry)

    lax.fori_loop(0, steps, one_step, 0)

    row, col = iota((128, 128), 0), iota((128, 128), 1)
    line = iota((8, 128), 0)
    spot = iota((8, 128), 1)
    height = place_ref[0]
    core = place_ref[1]

    def pack(out_ref, s, k):
        @pl.when(counts[k] == 0)
        def _():
            out_ref[s] = jnp.zeros((ROWS_SENT, 128), f32)

        @pl.when(counts[k] > 0)
        def _():
            upper = gram[k, 0:128, 0:128]
            lower = gram[k, 128:256, 128:256]
            upper = 0.5 * (upper + upper.T)
            lower = 0.5 * (lower + lower.T)
            cross = 0.5 * (gram[k, 128:256, 0:128] + gram[k, 0:128, 128:256].T)
            out_ref[s, 0:128, :] = jnp.where(col > row, upper, lower)
            out_ref[s, 128:256, :] = cross
            diagonal = jnp.sum(jnp.where(col == row, upper, 0.0), axis=0, keepdims=True)
            first = jnp.sum(fit[k, 0:128, :].T, axis=0, keepdims=True)
            second = jnp.sum(fit[k, 128:256, :].T, axis=0, keepdims=True)
            power = jnp.sum(energy[pl.ds(k, 1), :], axis=1, keepdims=True)
            number = counts[k].astype(f32)
            last = jnp.where(spot == 0, power, jnp.where(spot == 1, number, 0.0))
            rest = jnp.where(line == 3, last, 0.0)
            rest = jnp.where(line == 0, diagonal, rest)
            rest = jnp.where(line == 1, first, rest)
            out_ref[s, 256:264, :] = jnp.where(line == 2, second, rest)

    for s in range(4):
        base = 2 * ((height + s) & 3)
        pack(other_ref, s, base + 1 - core)
        pack(mine_ref, s, base + core)


def gram_parts(place, design, weight, residuals, slot_pulsar, slot_rows):
    slots = design.shape[0]
    piece = pltpu.VMEM((4, ROWS_SENT, 128), f32)
    smem = pl.BlockSpec(memory_space=pltpu.SMEM)
    vmem = pl.BlockSpec(memory_space=pltpu.VMEM)
    hbm = pl.BlockSpec(memory_space=pl.ANY)
    return pl.pallas_call(
        gram_kernel,
        in_specs=[smem, smem, smem, hbm, vmem, vmem],
        out_specs=[vmem, vmem],
        scratch_shapes=[
            pltpu.VMEM((slots, 128, COLUMNS), jnp.bfloat16),
            pltpu.VMEM((GROUP_PULSARS, COLUMNS, COLUMNS), f32),
            pltpu.VMEM((GROUP_PULSARS, COLUMNS, 128), f32),
            pltpu.VMEM((GROUP_PULSARS, 128), f32),
            pltpu.VMEM((slots, 128), f32),
            pltpu.SMEM((GROUP_PULSARS,), jnp.int32),
            pltpu.SemaphoreType.DMA((slots // STEP_BLOCKS,)),
        ],
        out_shape=[piece, piece],
        name="gram",
    )(slot_pulsar, slot_rows, place, design, weight, residuals)


def coupling_kernel(place_ref, directions_ref, out_ref):
    core = place_ref[1]
    row, col = iota((128, 128), 0), iota((128, 128), 1)
    source = jnp.where(col < 64, 2 * col + core, 2 * col - 127 - core)
    chosen = (row == source).astype(f32)
    lines = jnp.concatenate([directions_ref[...], jnp.zeros((5, 128), f32)], axis=0)
    lines = jnp.dot(lines, chosen, precision=highest, preferred_element_type=f32)
    turned = lines.T
    cosines = jnp.zeros((128, 128), f32)
    for i in range(3):
        cosines = cosines + turned[:, i : i + 1] * lines[i : i + 1, :]
    cosines = jnp.clip(cosines, -1.0, 1.0)
    same = row == col
    spread = jnp.where(same, 1.0, 0.5 * (1.0 - cosines))
    curve = 1.5 * spread * jnp.log(spread) - 0.25 * spread + 0.5
    correlation = jnp.where(same, 1.0, curve)
    identity = jnp.where(same, 1.0, 0.0)
    tiles = [
        [correlation[8 * a : 8 * a + 8, :], identity[8 * a : 8 * a + 8, :]] for a in range(16)
    ]
    tiles, _ = eliminate_rows(tiles, 0, jnp.zeros((8, 128), f32))
    for a in range(16):
        out_ref[8 * a : 8 * a + 8, :] = tiles[a][1]


def coupling_inverse(place, directions):
    return pl.pallas_call(
        coupling_kernel,
        in_specs=[
            pl.BlockSpec(memory_space=pltpu.SMEM),
            pl.BlockSpec(memory_space=pltpu.VMEM),
        ],
        out_specs=pl.BlockSpec(memory_space=pltpu.VMEM),
        out_shape=pltpu.VMEM((128, 128), f32),
        name="coupling",
    )(place, directions)


def power_column(spectrum_ref):
    inverse = 1.0 / spectrum_ref[...]
    half = iota((64, 32), 0) >> 1
    spread = jnp.where(iota((64, 32), 1) == half, jnp.broadcast_to(inverse, (64, 32)), 0.0)
    return jnp.sum(spread, axis=1, keepdims=True)


def own_kernel(
    place_ref,
    kept,
    part0,
    part1,
    part2,
    part3,
    prior_ref,
    spectrum_ref,
    coupling_ref,
    sent_ref,
    extra_ref,
    logdet_ref,
    work,
):
    row, col = iota((128, 128), 0), iota((128, 128), 1)

    def summed(lo, hi):
        near = kept[0, lo:hi, :] + part0[0, lo:hi, :]
        return (near + part1[lo:hi, :]) + (part2[lo:hi, :] + part3[lo:hi, :])

    packed = summed(0, 128)
    cross = summed(128, 256)
    rest = summed(256, 264)
    turned = packed.T
    prior = 1.0 / prior_ref[...]
    prior = jnp.concatenate([jnp.zeros((1, 64), f32), prior], axis=1)
    upper = jnp.where(col > row, packed, turned)
    upper = jnp.where(col == row, rest[0:1, :] + prior[:, 0:128], upper)
    lower = jnp.where(col <= row, packed, turned)
    lower = jnp.where(col == row, lower + prior[:, 128:256], lower)
    work[0:128, 0:128] = upper
    work[128:256, 128:256] = lower
    work[128:256, 0:128] = cross
    work[0:128, 128:256] = cross.T
    side = rest.T
    work[0:128, 256:384] = jnp.broadcast_to(side[:, 1:2], (128, 128))
    work[128:256, 256:384] = jnp.broadcast_to(side[:, 2:3], (128, 128))

    log_sum = jnp.zeros((8, 128), f32)
    quadratic = jnp.zeros((64, 128), f32)
    for panel in range(3):
        at = COMMON + 64 * panel
        old = work[at : at + 64, :]
        tiles = [
            [old[8 * a : 8 * a + 8, 128 * t : 128 * t + 128] for t in range(3)] for a in range(8)
        ]
        tiles, log_sum = eliminate_rows(tiles, at, log_sum)
        fresh = [jnp.concatenate([tiles[a][t] for a in range(8)], axis=0) for t in range(3)]
        quadratic = quadratic + old[:, 256:384] * fresh[2]
        final = panel == 2
        for t in (0,) if final else (0, 1):
            left = old[:, 128 * t : 128 * t + 128]
            for u in (0, 2) if final else (0, 1, 2):
                change = lax.dot_general(
                    left,
                    fresh[u],
                    (((0,), (0,)), ((), ())),
                    precision=highest,
                    preferred_element_type=f32,
                )
                where = (slice(128 * t, 128 * t + 128), slice(128 * u, 128 * u + 128))
                work[where] = work[where] - change

    own = place_ref[2]
    mine = jnp.where((row == own) & (col == own), coupling_ref[...], 0.0)
    self_coupling = total(mine)
    power = power_column(spectrum_ref)
    row64, col64 = iota((64, 128), 0), iota((64, 128), 1)
    block = work[0:64, 0:128]
    block = jnp.where(row64 == col64, block + self_coupling * power, block)
    block = jnp.where(col64 < 64, block, jnp.where(col64 == row64 + 64, 1.0, 0.0))
    tiles = [[block[8 * a : 8 * a + 8, :]] for a in range(8)]
    tiles, log_sum = eliminate_rows(tiles, 0, log_sum)
    solved = jnp.concatenate([tiles[a][0] for a in range(8)], axis=0)
    inverse = pltpu.roll(solved, 64, 1)
    top, bottom = inverse[0:32, :], inverse[32:64, :]
    row32, col32 = iota((32, 128), 0), iota((32, 128), 1)
    moved = pltpu.roll(bottom, 96, 1)
    triangle = jnp.where(col32 > row32, top, moved)
    folded = jnp.where(col32 < 32, triangle, top)
    lines = jnp.where(
        iota((16, 128), 1) < 64, folded[0:16, :], pltpu.roll(folded[16:32, :], 64, 1)
    )
    diagonal = jnp.sum(jnp.where(row32 == col32, top, 0.0), axis=0, keepdims=True)
    target = work[0:64, 256:384]
    target_line = jnp.concatenate([target, target], axis=0).T[0:1, :]
    final_line = jnp.where(iota((1, 128), 1) < 64, diagonal, target_line)
    whole = jnp.concatenate([lines, final_line], axis=0)
    whole = jnp.concatenate([whole] * 8, axis=0)
    for i in range(8):
        sent_ref[8 * LINES * i : 8 * LINES * (i + 1), :] = whole
    spent = jnp.sum(quadratic, axis=0, keepdims=True)
    left_over = rest[3:4, 0:1] - spent[:, 0:1]
    line = iota((8, 128), 0)
    extra_ref[...] = jnp.where(line == 0, left_over, rest[3:4, 1:2])
    logdet_ref[0] = log_sum[0, 0] / COLUMNS


def own_terms(place, parts, own_prior, spectrum, coupling):
    vmem = pl.BlockSpec(memory_space=pltpu.VMEM)
    smem = pl.BlockSpec(memory_space=pltpu.SMEM)
    return pl.pallas_call(
        own_kernel,
        in_specs=[smem] + [vmem] * 8,
        out_specs=[vmem, vmem, smem],
        out_shape=[
            pltpu.VMEM((64 * LINES, 128), f32),
            pltpu.VMEM((8, 128), f32),
            jax.ShapeDtypeStruct((1,), f32),
        ],
        scratch_shapes=[pltpu.VMEM((COLUMNS, 384), f32)],
        name="own",
    )(place, *map(in_vmem, parts), own_prior, spectrum, in_vmem(coupling))


def gradient_kernel(
    place_ref,
    near_ref,
    far_ref,
    coupling_ref,
    spectrum_ref,
    extra_ref,
    coeffs_ref,
    chi_ref,
    flat,
    inverse,
    resid,
    direction,
    mapped,
    answer,
    turned,
):
    for i in range(LINES):
        where = slice(128 * i, 128 * i + 128)
        rows = pl.ds(i, 64, stride=LINES)
        flat[where, :] = jnp.concatenate([near_ref[rows, :], far_ref[rows, :]], axis=0).T
    line = iota((8, 128), 0)

    def start(r):
        return (r % 16) * 128 + (r // 16) * 64

    def across(c, offset):
        return flat[pl.ds(start(c) + offset, 8, stride=128), :]

    for r in range(32):
        at = start(r)
        corner = flat[2048 + r : 2049 + r, :]
        for c in range(0, 32, 8):
            straight = None if c + 7 < r else flat[at + c : at + c + 8, :]
            crossed = None if c > r else across(c, r)
            if straight is None:
                first = second = crossed
                second = None
            if crossed is None:
                first = straight
            if straight is not None and crossed is not None:
                index = line + c
                first = jnp.where(index > r, straight, crossed)
                first = jnp.where(index == r, corner, first)
            inverse[r, c : c + 8, :] = first
            low = None if c > r else flat[at + c : at + c + 8, :]
            high = None if c + 7 <= r else across(c, r)
            if low is None:
                value = high
            elif high is None:
                value = low
            else:
                value = jnp.where(line + c <= r, low, high)
            inverse[32 + r, 32 + c : 40 + c, :] = value
            inverse[r, 32 + c : 40 + c, :] = flat[at + 32 + c : at + 40 + c, :]
            inverse[32 + r, c : c + 8, :] = across(c, 32 + r)

    row, col = iota((128, 128), 0), iota((128, 128), 1)
    mixing = jnp.where(row == col, 0.0, coupling_ref[...])
    power = power_column(spectrum_ref)
    resid[...] = flat[2112:2176, :]
    direction[...] = jnp.zeros((64, 128), f32)
    mapped[...] = jnp.zeros((64, 128), f32)
    answer[...] = jnp.zeros((64, 128), f32)

    def iterate(_, carry):
        inner, curved = carry
        now = resid[...]
        scaled = jnp.zeros((64, 128), f32)
        for k in range(64):
            scaled = scaled + inverse[k] * resid[k : k + 1, :]
        mixed = jnp.dot(scaled, mixing, precision=highest, preferred_element_type=f32)
        image = now + power * mixed
        old_mapped = mapped[...]
        inner_next = total(now * scaled)
        straight = total(scaled * image)
        crossing = total(scaled * old_mapped)
        ratio = inner_next / inner
        curved = straight + ratio * (2.0 * crossing + ratio * curved)
        step = inner_next / curved
        toward = scaled + ratio * direction[...]
        image = image + ratio * old_mapped
        direction[...] = toward
        mapped[...] = image
        answer[...] = answer[...] + step * toward
        resid[...] = now - step * image
        return inner_next, curved

    lax.fori_loop(0, ITERS, iterate, (jnp.ones((1, 1), f32), jnp.zeros((1, 1), f32)))
    own = place_ref[2]
    value = answer[...]
    gained = jnp.sum(flat[2112:2176, :] * value, axis=0, keepdims=True)
    lane = iota((1, 128), 1)
    gained = jnp.sum(jnp.where(lane == own, gained, 0.0), axis=1, keepdims=True)
    chi = (extra_ref[0:1, 0:1] - gained) / extra_ref[1:2, 0:1]
    chi_ref[0] = chi[0, 0]
    turned[...] = jnp.concatenate([value, value], axis=0).T
    coeffs_ref[...] = turned[pl.ds(own, 1), :][:, 0:64]


def conjugate(place, near, far, coupling, spectrum, extra):
    vmem = pl.BlockSpec(memory_space=pltpu.VMEM)
    smem = pl.BlockSpec(memory_space=pltpu.SMEM)
    square = pltpu.VMEM((64, 128), f32)
    return pl.pallas_call(
        gradient_kernel,
        in_specs=[smem] + [vmem] * 5,
        out_specs=[vmem, smem],
        out_shape=[jax.ShapeDtypeStruct((1, COMMON), f32), jax.ShapeDtypeStruct((1,), f32)],
        scratch_shapes=[
            pltpu.VMEM((WIDTH, 128), f32),
            pltpu.VMEM((64, 64, 128), f32),
            square,
            square,
            square,
            square,
            pltpu.VMEM((128, 128), f32),
        ],
        name="gradient",
    )(place, in_vmem(near), in_vmem(far), in_vmem(coupling), spectrum, in_vmem(extra))


def body(design, noise_weight, residuals, slot_pulsar, slot_rows, own_prior, spectrum, directions):
    toa = lax.axis_index("toa")
    device = lax.axis_index("psr") * lax.axis_size("toa") + toa
    count = lax.axis_size("psr") * lax.axis_size("toa")
    core = toa % 2
    place = jnp.stack([toa // 2, core, device // 2]).astype(jnp.int32)
    spectrum = spectrum.reshape(1, -1)
    mine, other = gram_parts(place, design, noise_weight, residuals, slot_pulsar, slot_rows)
    got = lax.ppermute(other, "toa", [(u, u ^ 1) for u in range(8)])
    parts = [mine, got]
    for s in range(1, 4):
        part = mine[s] + got[s]
        parts.append(lax.ppermute(part, "toa", [(u, (u + 2 * s) % 8) for u in range(8)]))
    coupling = coupling_inverse(place, directions)
    sent, extra, log_dets = own_terms(place, parts, own_prior, spectrum, coupling)
    groups = [list(range(c, count, 2)) for c in range(2)]
    sent = sent.reshape(64, 1, WIDTH)
    near = lax.all_to_all(sent, AXES, 0, 0, tiled=True, axis_index_groups=groups)
    near = near.reshape(64 * LINES, 128)
    far = lax.ppermute(near, "toa", [(u, u ^ 1) for u in range(8)])
    coeffs, chi_square = conjugate(place, near, far, coupling, spectrum, extra)
    return (coeffs, log_dets, chi_square)


def solution(mesh):
    return jax.shard_map(
        body,
        mesh=mesh,
        in_specs=(
            P(AXES, None, None),
            P(AXES, None),
            P(AXES, None),
            P(AXES),
            P(AXES),
            P(AXES, None),
            P(),
            P(),
        ),
        out_specs=(P(AXES, None), P(AXES), P(AXES)),
        check_vma=False,
    )
```

```python
import jax
import jax.numpy as jnp
from jax import lax
from jax.experimental import pallas as pl
from jax.experimental.pallas import tpu as pltpu
from jax.sharding import PartitionSpec as P

GROUP_PULSARS = 8
ITERS = 8
COLUMNS = 256
COMMON = 64
STEP_BLOCKS = 8
ROWS_SENT = 264
AHEAD = True
WIDTH = 2176
LINES = WIDTH // 128
AXES = ("psr", "toa")

highest = lax.Precision.HIGHEST
f32 = jnp.float32


def location():
    toa = lax.axis_index("toa")
    return toa >> 1, toa & 1, lax.axis_index("psr") * 4 + (toa >> 1)


def in_vmem(value):
    return pltpu.with_memory_space_constraint(value, pltpu.VMEM)


def iota(shape, dim):
    return lax.broadcasted_iota(jnp.int32, shape, dim)


def sub_bcast(value, row):
    return jnp.broadcast_to(value[row : row + 1, :], value.shape)


def lane_bcast(value, lane):
    index = jnp.full(value.shape, lane, jnp.int32)
    return jnp.take_along_axis(value, index, axis=1, mode="promise_in_bounds")


def total(value):
    return jnp.sum(jnp.sum(value, axis=0, keepdims=True), axis=1, keepdims=True)


def summed_tree(parts):
    while len(parts) > 1:
        joined = [u + v for u, v in zip(parts[::2], parts[1::2])]
        parts = joined + ([parts[-1]] if len(parts) % 2 else [])
    return parts[0]


def invert_block(cols, log_sum):
    row = iota((8, 128), 0)
    for i in range(0, 8, 2):
        first, second = row == i, row == i + 1
        c0, c1 = cols[i], cols[i + 1]
        p, q = sub_bcast(c0, i), sub_bcast(c1, i)
        r, s = sub_bcast(c0, i + 1), sub_bcast(c1, i + 1)
        det = p * s - q * r
        inverse = 1.0 / det
        log_sum = log_sum + jnp.log(det)
        for k in range(8):
            if k not in (i, i + 1):
                u, v = sub_bcast(cols[k], i), sub_bcast(cols[k], i + 1)
                n0 = s * u - q * v
                n1 = p * v - r * u
                moved = cols[k] - (c0 * n0 + c1 * n1) * inverse
                moved = jnp.where(first, n0 * inverse, moved)
                cols[k] = jnp.where(second, n1 * inverse, moved)
        left = jnp.where(first, s, jnp.where(second, -r, c1 * r - c0 * s))
        right = jnp.where(first, -q, jnp.where(second, p, c0 * q - c1 * p))
        cols[i] = left * inverse
        cols[i + 1] = right * inverse
    return cols, log_sum


class Board:
    def __init__(self, ref):
        self.ref, self.used = ref, 0

    def rows(self, value):
        at = self.used
        self.used = at + 1
        self.ref[at] = value
        return [self.ref[at, k : k + 1, :] for k in range(8)]


def eliminate_rows(tiles, first_lane, log_sum, board, whole, ahead=True):
    count = len(tiles)
    width = len(tiles[0])
    before, after = [], []

    def columns(a, b):
        at = first_lane + 8 * b
        return [lane_bcast(tiles[a][at // 128], at % 128 + k) for k in range(8)]

    cols = columns(0, 0)
    for b in range(count):
        cols, log_sum = invert_block(cols, log_sum)
        last = b + 1 == count
        factors = {}
        if not last and ahead:
            factor = columns(b + 1, b)
            factors[b + 1] = factor
            coming = columns(b + 1, b + 1)
            spots = [board.rows(value) for value in factor]
            for j in range(8):
                solved = summed_tree([cols[m] * spots[m][j] for m in range(8)])
                change = summed_tree([factor[k] * sub_bcast(solved, k) for k in range(8)])
                coming[j] = coming[j] - change
        fresh, spread = [], []
        for t in range(width):
            rows = board.rows(tiles[b][t])
            fresh.append(summed_tree([cols[k] * rows[k] for k in range(8)]))
            spread.append(board.rows(fresh[t]))
        before.append(tiles[b])
        after.append(fresh)
        for a in range(0 if whole else b + 1, count):
            if a != b:
                factor = factors[a] if a in factors else columns(a, b)
                tiles[a] = [
                    tiles[a][t] - summed_tree([factor[k] * spread[t][k] for k in range(8)])
                    for t in range(width)
                ]
        if whole:
            tiles[b] = fresh
        if not last:
            cols = coming if ahead else columns(b + 1, b + 1)
    return tiles, before, after, log_sum


def gram_kernel(
    pulsar_ref,
    rows_ref,
    design_ref,
    weight_ref,
    resid_ref,
    mine_ref,
    other_ref,
    blocks,
    gram,
    fit,
    energy,
    wide_resid,
    counts,
    arrived,
):
    slots = weight_ref.shape[0]
    steps = slots // STEP_BLOCKS

    def load(step):
        where = pl.ds(step * STEP_BLOCKS, STEP_BLOCKS)
        return pltpu.make_async_copy(design_ref.at[where], blocks.at[where], arrived.at[step])

    for step in range(steps):
        load(step).start()
    gram[...] = jnp.zeros(gram.shape, f32)
    fit[...] = jnp.zeros(fit.shape, f32)
    energy[...] = jnp.zeros(energy.shape, f32)
    for k in range(GROUP_PULSARS):
        counts[k] = 0
    wide_resid[...] = resid_ref[...].astype(f32)
    lane = iota((1, 128), 1)

    def one_step(step, carry):
        load(step).wait()
        at = step * STEP_BLOCKS
        pulsars = [pulsar_ref[at + i] for i in range(STEP_BLOCKS)]
        rows = [rows_ref[at + i] for i in range(STEP_BLOCKS)]
        same = pulsars[1] == pulsars[0]
        for i in range(2, STEP_BLOCKS):
            same = same & (pulsars[i] == pulsars[0])
        low = jnp.where(same, pulsars[0], 0)
        high = jnp.where(same, pulsars[0] + 1, GROUP_PULSARS)

        def one_pulsar(pulsar, carry):
            valid = [jnp.where(pulsars[i] == pulsar, rows[i], 0) for i in range(STEP_BLOCKS)]
            number = valid[0]
            for i in range(1, STEP_BLOCKS):
                number = number + valid[i]

            @pl.when(number > 0)
            def _():
                pieces, fitted, squares = [], None, None
                for i in range(STEP_BLOCKS):
                    weight = jnp.where(lane < valid[i], weight_ref[pl.ds(at + i, 1), :], 0.0)
                    resid = wide_resid[pl.ds(at + i, 1), :]
                    turned = blocks[at + i].T.astype(f32)
                    weighted = (turned * weight).astype(jnp.bfloat16)
                    pieces.append(weighted)
                    product = weighted.astype(f32) * resid
                    square = weight * resid * resid
                    fitted = product if fitted is None else fitted + product
                    squares = square if squares is None else squares + square
                left = jnp.concatenate(pieces, axis=1)
                right = blocks[pl.ds(at, STEP_BLOCKS)].reshape(STEP_BLOCKS * 128, COLUMNS)
                gram[pulsar] = gram[pulsar] + jnp.dot(left, right, preferred_element_type=f32)
                fit[pulsar] = fit[pulsar] + fitted
                energy[pl.ds(pulsar, 1), :] = energy[pl.ds(pulsar, 1), :] + squares
                counts[pulsar] = counts[pulsar] + number

            return carry

        return lax.fori_loop(low, high, one_pulsar, carry)

    lax.fori_loop(0, steps, one_step, 0)

    row, col = iota((128, 128), 0), iota((128, 128), 1)
    line = iota((8, 128), 0)
    spot = iota((8, 128), 1)
    height, core, _ = location()

    def pack(out_ref, s, k):
        @pl.when(counts[k] == 0)
        def _():
            out_ref[s] = jnp.zeros((ROWS_SENT, 128), f32)

        @pl.when(counts[k] > 0)
        def _():
            upper = gram[k, 0:128, 0:128]
            lower = gram[k, 128:256, 128:256]
            upper = 0.5 * (upper + upper.T)
            lower = 0.5 * (lower + lower.T)
            cross = 0.5 * (gram[k, 128:256, 0:128] + gram[k, 0:128, 128:256].T)
            out_ref[s, 0:128, :] = jnp.where(col > row, upper, lower)
            out_ref[s, 128:256, :] = cross
            diagonal = jnp.sum(jnp.where(col == row, upper, 0.0), axis=0, keepdims=True)
            first = jnp.sum(fit[k, 0:128, :].T, axis=0, keepdims=True)
            second = jnp.sum(fit[k, 128:256, :].T, axis=0, keepdims=True)
            power = jnp.sum(energy[pl.ds(k, 1), :], axis=1, keepdims=True)
            number = counts[k].astype(f32)
            last = jnp.where(spot == 0, power, jnp.where(spot == 1, number, 0.0))
            rest = jnp.where(line == 3, last, 0.0)
            rest = jnp.where(line == 0, diagonal, rest)
            rest = jnp.where(line == 1, first, rest)
            out_ref[s, 256:264, :] = jnp.where(line == 2, second, rest)

    for s in range(4):
        base = 2 * ((height + s) & 3)
        pack(other_ref, s, base + 1 - core)
        pack(mine_ref, s, base + core)


def gram_parts(design, weight, residuals, slot_pulsar, slot_rows):
    slots = design.shape[0]
    piece = pltpu.VMEM((4, ROWS_SENT, 128), f32)
    smem = pl.BlockSpec(memory_space=pltpu.SMEM)
    vmem = pl.BlockSpec(memory_space=pltpu.VMEM)
    hbm = pl.BlockSpec(memory_space=pl.ANY)
    return pl.pallas_call(
        gram_kernel,
        in_specs=[smem, smem, hbm, vmem, vmem],
        out_specs=[vmem, vmem],
        scratch_shapes=[
            pltpu.VMEM((slots, 128, COLUMNS), jnp.bfloat16),
            pltpu.VMEM((GROUP_PULSARS, COLUMNS, COLUMNS), f32),
            pltpu.VMEM((GROUP_PULSARS, COLUMNS, 128), f32),
            pltpu.VMEM((GROUP_PULSARS, 128), f32),
            pltpu.VMEM((slots, 128), f32),
            pltpu.SMEM((GROUP_PULSARS,), jnp.int32),
            pltpu.SemaphoreType.DMA((slots // STEP_BLOCKS,)),
        ],
        out_shape=[piece, piece],
        name="gram",
    )(slot_pulsar, slot_rows, design, weight, residuals)


def coupling_kernel(directions_ref, out_ref, board_ref):
    _, core, _ = location()
    row, col = iota((128, 128), 0), iota((128, 128), 1)
    source = jnp.where(col < 64, 2 * col + core, 2 * col - 127 - core)
    chosen = (row == source).astype(f32)
    lines = jnp.concatenate([directions_ref[...], jnp.zeros((5, 128), f32)], axis=0)
    lines = jnp.dot(lines, chosen, precision=highest, preferred_element_type=f32)
    turned = lines.T
    cosines = jnp.zeros((128, 128), f32)
    for i in range(3):
        cosines = cosines + turned[:, i : i + 1] * lines[i : i + 1, :]
    cosines = jnp.clip(cosines, -1.0, 1.0)
    same = row == col
    spread = jnp.where(same, 1.0, 0.5 * (1.0 - cosines))
    curve = 1.5 * spread * jnp.log(spread) - 0.25 * spread + 0.5
    correlation = jnp.where(same, 1.0, curve)
    identity = jnp.where(same, 1.0, 0.0)
    tiles = [
        [correlation[8 * a : 8 * a + 8, :], identity[8 * a : 8 * a + 8, :]] for a in range(16)
    ]
    board = Board(board_ref)
    tiles, _, _, _ = eliminate_rows(tiles, 0, jnp.zeros((8, 128), f32), board, True, AHEAD)
    for a in range(16):
        out_ref[8 * a : 8 * a + 8, :] = tiles[a][1]


def coupling_inverse(directions):
    return pl.pallas_call(
        coupling_kernel,
        in_specs=[pl.BlockSpec(memory_space=pltpu.VMEM)],
        out_specs=pl.BlockSpec(memory_space=pltpu.VMEM),
        out_shape=pltpu.VMEM((128, 128), f32),
        scratch_shapes=[pltpu.VMEM((16 * 12, 8, 128), f32)],
        name="coupling",
    )(directions)


def power_column(spectrum_ref):
    inverse = 1.0 / spectrum_ref[...]
    half = iota((64, 32), 0) >> 1
    spread = jnp.where(iota((64, 32), 1) == half, jnp.broadcast_to(inverse, (64, 32)), 0.0)
    return jnp.sum(spread, axis=1, keepdims=True)


def own_kernel(
    kept,
    part0,
    part1,
    part2,
    part3,
    prior_ref,
    spectrum_ref,
    coupling_ref,
    sent_ref,
    extra_ref,
    logdet_ref,
    board_ref,
):
    row, col = iota((128, 128), 0), iota((128, 128), 1)

    def summed(lo, hi):
        near = kept[0, lo:hi, :] + part0[0, lo:hi, :]
        return (near + part1[lo:hi, :]) + (part2[lo:hi, :] + part3[lo:hi, :])

    packed = summed(0, 128)
    cross = summed(128, 256)
    rest = summed(256, 264)
    turned = packed.T
    prior = 1.0 / prior_ref[...]
    prior = jnp.concatenate([jnp.zeros((1, 64), f32), prior], axis=1)
    upper = jnp.where(col > row, packed, turned)
    upper = jnp.where(col == row, rest[0:1, :] + prior[:, 0:128], upper)
    lower = jnp.where(col <= row, packed, turned)
    lower = jnp.where(col == row, lower + prior[:, 128:256], lower)
    side = rest.T
    lane = iota((64, 128), 1)
    log_sum = jnp.zeros((8, 128), f32)

    board = Board(board_ref)

    def panel_of(parts, at, log_sum):
        tiles = [[part[8 * a : 8 * a + 8, :] for part in parts] for a in range(8)]
        _, before, after, log_sum = eliminate_rows(tiles, at, log_sum, board, False)
        old, new = [
            [jnp.concatenate([rows[a][t] for a in range(8)], axis=0) for t in range(len(parts))]
            for rows in (before, after)
        ]
        return old, new, log_sum

    def product(left, right):
        return lax.dot_general(
            left,
            right,
            (((0,), (0,)), ((), ())),
            precision=highest,
            preferred_element_type=f32,
        )

    turned_cross = cross.T
    right_top = jnp.broadcast_to(side[:, 1:2], (128, 128))
    right_low = jnp.broadcast_to(side[:, 2:3], (128, 128))
    final = jnp.where(lane < 64, upper[0:64, :], right_top[0:64, :])
    low = [jnp.where(iota((128, 128), 1) < 64, cross, right_low), lower]

    parts = [upper[64:128, :], turned_cross[64:128, :], right_top[64:128, :]]
    old, fresh, log_sum = panel_of(parts, 64, log_sum)
    quadratic = old[2] * fresh[2]
    first = jnp.where(lane < 64, fresh[0], fresh[2])
    change = product(old[1], jnp.concatenate([first, fresh[1]], axis=1))
    low = [low[0] - change[:, 0:128], low[1] - change[:, 128:256]]
    final = final - product(old[0][:, 0:64], first)

    parts = [low[0][0:64, :], low[1][0:64, :]]
    old, fresh, log_sum = panel_of(parts, 128, log_sum)
    quadratic = quadratic + old[0] * fresh[0]
    change = product(old[1][:, 64:128], jnp.concatenate(fresh, axis=1))
    final = final - product(old[0][:, 0:64], fresh[0])

    parts = [low[0][64:128, :] - change[:, 0:128], low[1][64:128, :] - change[:, 128:256]]
    old, fresh, log_sum = panel_of(parts, 192, log_sum)
    quadratic = quadratic + old[0] * fresh[0]
    final = final - product(old[0][:, 0:64], fresh[0])

    _, _, own = location()
    mine = jnp.where((row == own) & (col == own), coupling_ref[...], 0.0)
    self_coupling = total(mine)
    power = power_column(spectrum_ref)
    row64, col64 = iota((64, 128), 0), iota((64, 128), 1)
    block = final
    block = jnp.where(row64 == col64, block + self_coupling * power, block)
    block = jnp.where(col64 < 64, block, jnp.where(col64 == row64 + 64, 1.0, 0.0))
    tiles = [[block[8 * a : 8 * a + 8, :]] for a in range(8)]
    tiles, _, _, log_sum = eliminate_rows(tiles, 0, log_sum, board, True)
    solved = jnp.concatenate([tiles[a][0] for a in range(8)], axis=0)
    inverse = pltpu.roll(solved, 64, 1)
    top, bottom = inverse[0:32, :], inverse[32:64, :]
    row32, col32 = iota((32, 128), 0), iota((32, 128), 1)
    moved = pltpu.roll(bottom, 96, 1)
    triangle = jnp.where(col32 > row32, top, moved)
    folded = jnp.where(col32 < 32, triangle, top)
    lines = jnp.where(
        iota((16, 128), 1) < 64, folded[0:16, :], pltpu.roll(folded[16:32, :], 64, 1)
    )
    diagonal = jnp.sum(jnp.where(row32 == col32, top, 0.0), axis=0, keepdims=True)
    target = final
    target_line = jnp.concatenate([target, target], axis=0).T[64:65, :]
    final_line = jnp.where(iota((1, 128), 1) < 64, diagonal, target_line)
    whole = jnp.concatenate([lines, final_line], axis=0)
    whole = jnp.concatenate([whole] * 8, axis=0)
    for i in range(8):
        sent_ref[8 * LINES * i : 8 * LINES * (i + 1), :] = whole
    spent = jnp.sum(quadratic, axis=0, keepdims=True)
    left_over = rest[3:4, 0:1] - spent[:, 64:65]
    line = iota((8, 128), 0)
    extra_ref[...] = jnp.where(line == 0, left_over, rest[3:4, 1:2])
    logdet_ref[0] = log_sum[0, 0] / COLUMNS


def own_terms(parts, own_prior, spectrum, coupling):
    vmem = pl.BlockSpec(memory_space=pltpu.VMEM)
    smem = pl.BlockSpec(memory_space=pltpu.SMEM)
    return pl.pallas_call(
        own_kernel,
        in_specs=[vmem] * 8,
        out_specs=[vmem, vmem, smem],
        out_shape=[
            pltpu.VMEM((64 * LINES, 128), f32),
            pltpu.VMEM((8, 128), f32),
            jax.ShapeDtypeStruct((1,), f32),
        ],
        scratch_shapes=[pltpu.VMEM((32 * 14, 8, 128), f32)],
        name="own",
    )(*map(in_vmem, parts), own_prior, spectrum, in_vmem(coupling))


def gradient_kernel(
    near_ref,
    far_ref,
    coupling_ref,
    spectrum_ref,
    extra_ref,
    coeffs_ref,
    chi_ref,
    flat,
    inverse,
    target,
    resid,
    direction,
    mapped,
    answer,
    turned,
):
    for i in range(LINES):
        rows = pl.ds(i, 64, stride=LINES)
        both = jnp.concatenate([near_ref[rows, :], far_ref[rows, :]], axis=0).T
        for m in range(0, 128, 8):
            flat[pl.ds(m * LINES + i, 8, stride=LINES), :] = both[m : m + 8, :]
    line = iota((8, 128), 0)

    def straight_of(r, c):
        return flat[pl.ds((64 * (r // 16) + c) * LINES + r % 16, 8, stride=LINES), :]

    def crossed_of(c, r):
        at = (64 * (c // 16) + r) * LINES + c % 16
        return flat[at : at + 8, :]

    for r in range(32):
        corner = flat[r * LINES + 16 : r * LINES + 17, :]
        for c in range(0, 32, 8):
            if c > r:
                upper, lower = straight_of(r, c), crossed_of(c, r)
            elif c + 7 < r:
                upper, lower = crossed_of(c, r), straight_of(r, c)
            else:
                index = line + c
                straight, crossed = straight_of(r, c), crossed_of(c, r)
                upper = jnp.where(index > r, straight, crossed)
                upper = jnp.where(index == r, corner, upper)
                lower = jnp.where(index <= r, straight, crossed)
            inverse[r, c : c + 8, :] = upper
            inverse[32 + r, 32 + c : 40 + c, :] = lower
            inverse[r, 32 + c : 40 + c, :] = straight_of(r, 32 + c)
            inverse[32 + r, c : c + 8, :] = crossed_of(c, 32 + r)
    for c in range(0, 64, 8):
        target[c : c + 8, :] = flat[pl.ds((64 + c) * LINES + 16, 8, stride=LINES), :]

    row, col = iota((128, 128), 0), iota((128, 128), 1)
    mixing = jnp.where(row == col, 0.0, coupling_ref[...])
    power = power_column(spectrum_ref)
    resid[...] = target[...]
    direction[...] = jnp.zeros((64, 128), f32)
    mapped[...] = jnp.zeros((64, 128), f32)
    answer[...] = jnp.zeros((64, 128), f32)

    def iterate(_, carry):
        inner, curved = carry
        now = resid[...]
        scaled = jnp.zeros((64, 128), f32)
        for k in range(64):
            scaled = scaled + inverse[k] * resid[k : k + 1, :]
        mixed = jnp.dot(scaled, mixing, precision=highest, preferred_element_type=f32)
        image = now + power * mixed
        old_mapped = mapped[...]
        inner_next = total(now * scaled)
        straight = total(scaled * image)
        crossing = total(scaled * old_mapped)
        ratio = inner_next / inner
        curved = straight + ratio * (2.0 * crossing + ratio * curved)
        step = inner_next / curved
        toward = scaled + ratio * direction[...]
        image = image + ratio * old_mapped
        direction[...] = toward
        mapped[...] = image
        answer[...] = answer[...] + step * toward
        resid[...] = now - step * image
        return inner_next, curved

    lax.fori_loop(0, ITERS, iterate, (jnp.ones((1, 1), f32), jnp.zeros((1, 1), f32)))
    _, _, own = location()
    value = answer[...]
    gained = jnp.sum(target[...] * value, axis=0, keepdims=True)
    lane = iota((1, 128), 1)
    gained = jnp.sum(jnp.where(lane == own, gained, 0.0), axis=1, keepdims=True)
    chi = (extra_ref[0:1, 0:1] - gained) / extra_ref[1:2, 0:1]
    chi_ref[0] = chi[0, 0]
    turned[...] = jnp.concatenate([value, value], axis=0).T
    coeffs_ref[...] = turned[pl.ds(own, 1), :][:, 0:64]


def conjugate(near, far, coupling, spectrum, extra):
    vmem = pl.BlockSpec(memory_space=pltpu.VMEM)
    smem = pl.BlockSpec(memory_space=pltpu.SMEM)
    square = pltpu.VMEM((64, 128), f32)
    return pl.pallas_call(
        gradient_kernel,
        in_specs=[vmem] * 5,
        out_specs=[vmem, smem],
        out_shape=[jax.ShapeDtypeStruct((1, COMMON), f32), jax.ShapeDtypeStruct((1,), f32)],
        scratch_shapes=[
            pltpu.VMEM((WIDTH, 128), f32),
            pltpu.VMEM((64, 64, 128), f32),
            square,
            square,
            square,
            square,
            square,
            pltpu.VMEM((128, 128), f32),
        ],
        name="gradient",
    )(in_vmem(near), in_vmem(far), in_vmem(coupling), spectrum, in_vmem(extra))


def body(design, noise_weight, residuals, slot_pulsar, slot_rows, own_prior, spectrum, directions):
    count = lax.axis_size("psr") * lax.axis_size("toa")
    spectrum = spectrum.reshape(1, -1)
    mine, other = gram_parts(design, noise_weight, residuals, slot_pulsar, slot_rows)
    got = lax.ppermute(other, "toa", [(u, u ^ 1) for u in range(8)])
    parts = [mine, got]
    for s in range(1, 4):
        part = mine[s] + got[s]
        parts.append(lax.ppermute(part, "toa", [(u, (u + 2 * s) % 8) for u in range(8)]))
    coupling = coupling_inverse(directions)
    sent, extra, log_dets = own_terms(parts, own_prior, spectrum, coupling)
    groups = [list(range(c, count, 2)) for c in range(2)]
    sent = sent.reshape(64, 1, WIDTH)
    near = lax.all_to_all(sent, AXES, 0, 0, tiled=True, axis_index_groups=groups)
    near = near.reshape(64 * LINES, 128)
    far = lax.ppermute(near, "toa", [(u, u ^ 1) for u in range(8)])
    coeffs, chi_square = conjugate(near, far, coupling, spectrum, extra)
    return (coeffs, log_dets, chi_square)


def solution(mesh):
    return jax.shard_map(
        body,
        mesh=mesh,
        in_specs=(
            P(AXES, None, None),
            P(AXES, None),
            P(AXES, None),
            P(AXES),
            P(AXES),
            P(AXES, None),
            P(),
            P(),
        ),
        out_specs=(P(AXES, None), P(AXES), P(AXES)),
        check_vma=False,
    )
```

```python
import jax
import jax.numpy as jnp
from jax import lax
from jax.experimental import pallas as pl
from jax.experimental.pallas import tpu as pltpu
from jax.sharding import PartitionSpec as P

GROUP_PULSARS = 8
ITERS = 8
COLUMNS = 256
COMMON = 64
STEP_BLOCKS = 8
IN_FLIGHT = 4
ROWS_SENT = 264
AHEAD = True
WIDTH = 2176
LINES = WIDTH // 128
AXES = ("psr", "toa")

highest = lax.Precision.HIGHEST
f32 = jnp.float32


def location():
    toa = lax.axis_index("toa")
    return toa >> 1, toa & 1, lax.axis_index("psr") * 4 + (toa >> 1)


def in_vmem(value):
    return pltpu.with_memory_space_constraint(value, pltpu.VMEM)


def iota(shape, dim):
    return lax.broadcasted_iota(jnp.int32, shape, dim)


def sub_bcast(value, row):
    return jnp.broadcast_to(value[row : row + 1, :], value.shape)


def lane_bcast(value, lane):
    index = jnp.full(value.shape, lane, jnp.int32)
    return jnp.take_along_axis(value, index, axis=1, mode="promise_in_bounds")


def total(value):
    return jnp.sum(jnp.sum(value, axis=0, keepdims=True), axis=1, keepdims=True)


def summed_tree(parts):
    while len(parts) > 1:
        joined = [u + v for u, v in zip(parts[::2], parts[1::2])]
        parts = joined + ([parts[-1]] if len(parts) % 2 else [])
    return parts[0]


def invert_block(cols, log_sum):
    row = iota((8, 128), 0)
    for i in range(0, 8, 2):
        first, second = row == i, row == i + 1
        c0, c1 = cols[i], cols[i + 1]
        p, q = sub_bcast(c0, i), sub_bcast(c1, i)
        r, s = sub_bcast(c0, i + 1), sub_bcast(c1, i + 1)
        det = p * s - q * r
        inverse = 1.0 / det
        log_sum = log_sum + jnp.log(det)
        for k in range(8):
            if k not in (i, i + 1):
                u, v = sub_bcast(cols[k], i), sub_bcast(cols[k], i + 1)
                n0 = s * u - q * v
                n1 = p * v - r * u
                moved = cols[k] - (c0 * n0 + c1 * n1) * inverse
                moved = jnp.where(first, n0 * inverse, moved)
                cols[k] = jnp.where(second, n1 * inverse, moved)
        left = jnp.where(first, s, jnp.where(second, -r, c1 * r - c0 * s))
        right = jnp.where(first, -q, jnp.where(second, p, c0 * q - c1 * p))
        cols[i] = left * inverse
        cols[i + 1] = right * inverse
    return cols, log_sum


class Board:
    def __init__(self, ref):
        self.ref, self.used = ref, 0

    def rows(self, value):
        at = self.used
        self.used = at + 1
        self.ref[at] = value
        return [self.ref[at, k : k + 1, :] for k in range(8)]


def eliminate_rows(tiles, first_lane, log_sum, board, whole, ahead=True):
    count = len(tiles)
    width = len(tiles[0])
    before, after = [], []

    def columns(a, b):
        at = first_lane + 8 * b
        return [lane_bcast(tiles[a][at // 128], at % 128 + k) for k in range(8)]

    cols = columns(0, 0)
    for b in range(count):
        cols, log_sum = invert_block(cols, log_sum)
        last = b + 1 == count
        factors = {}
        if not last and ahead:
            factor = columns(b + 1, b)
            factors[b + 1] = factor
            coming = columns(b + 1, b + 1)
            spots = [board.rows(value) for value in factor]
            for j in range(8):
                solved = summed_tree([cols[m] * spots[m][j] for m in range(8)])
                change = summed_tree([factor[k] * sub_bcast(solved, k) for k in range(8)])
                coming[j] = coming[j] - change
        fresh, spread = [], []
        for t in range(width):
            rows = board.rows(tiles[b][t])
            fresh.append(summed_tree([cols[k] * rows[k] for k in range(8)]))
            spread.append(board.rows(fresh[t]))
        before.append(tiles[b])
        after.append(fresh)
        for a in range(0 if whole else b + 1, count):
            if a != b:
                factor = factors[a] if a in factors else columns(a, b)
                tiles[a] = [
                    tiles[a][t] - summed_tree([factor[k] * spread[t][k] for k in range(8)])
                    for t in range(width)
                ]
        if whole:
            tiles[b] = fresh
        if not last:
            cols = coming if ahead else columns(b + 1, b + 1)
    return tiles, before, after, log_sum


def gram_kernel(
    pulsar_ref,
    rows_ref,
    design_ref,
    weight_ref,
    resid_ref,
    other_ref,
    gram,
    fit,
    energy,
    counts,
    blocks,
    turned,
    wide_resid,
    arrived,
):
    slots = weight_ref.shape[0]
    steps = slots // STEP_BLOCKS

    def load(step):
        where = pl.ds(step * STEP_BLOCKS, STEP_BLOCKS)
        return pltpu.make_async_copy(design_ref.at[where], blocks.at[where], arrived.at[step])

    def turn(step):
        load(step).wait()
        for i in range(STEP_BLOCKS):
            turned[step & 1, :, 128 * i : 128 * i + 128] = blocks[step * STEP_BLOCKS + i].T

    for step in range(IN_FLIGHT):
        load(step).start()
    gram[...] = jnp.zeros(gram.shape, f32)
    fit[...] = jnp.zeros(fit.shape, f32)
    energy[...] = jnp.zeros(energy.shape, f32)
    for k in range(GROUP_PULSARS):
        counts[k] = 0
    wide_resid[...] = resid_ref[...].astype(f32)
    lane = iota((1, 128), 1)
    turn(0)

    def one_step(step, carry):
        at = step * STEP_BLOCKS
        pulsars = [pulsar_ref[at + i] for i in range(STEP_BLOCKS)]
        rows = [rows_ref[at + i] for i in range(STEP_BLOCKS)]
        same = pulsars[1] == pulsars[0]
        for i in range(2, STEP_BLOCKS):
            same = same & (pulsars[i] == pulsars[0])
        low = jnp.where(same, pulsars[0], 0)
        high = jnp.where(same, pulsars[0] + 1, GROUP_PULSARS)
        following = jnp.minimum(step + 1, steps - 1)

        @pl.when(step + IN_FLIGHT < steps)
        def _():
            load(step + IN_FLIGHT).start()

        @pl.when(step + 1 < steps)
        def _():
            load(following).wait()

        def turn_next():
            for i in range(STEP_BLOCKS):
                block = blocks[following * STEP_BLOCKS + i]
                turned[(step + 1) & 1, :, 128 * i : 128 * i + 128] = block.T

        def one_pulsar(pulsar, carry):
            valid = [jnp.where(pulsars[i] == pulsar, rows[i], 0) for i in range(STEP_BLOCKS)]
            number = sum(valid[1:], valid[0])

            @pl.when(number > 0)
            def _():
                pieces, fitted, squares = [], None, None
                for i in range(STEP_BLOCKS):
                    weight = jnp.where(lane < valid[i], weight_ref[pl.ds(at + i, 1), :], 0.0)
                    resid = wide_resid[pl.ds(at + i, 1), :]
                    block = turned[step & 1, :, 128 * i : 128 * i + 128].astype(f32)
                    weighted = (block * weight).astype(jnp.bfloat16)
                    pieces.append(weighted)
                    product = weighted.astype(f32) * resid
                    square = weight * resid * resid
                    fitted = product if fitted is None else fitted + product
                    squares = square if squares is None else squares + square
                left = jnp.concatenate(pieces, axis=1)
                right = blocks[pl.ds(at, STEP_BLOCKS)].reshape(STEP_BLOCKS * 128, COLUMNS)
                gram[pulsar] = gram[pulsar] + jnp.dot(left, right, preferred_element_type=f32)
                fit[pulsar] = fit[pulsar] + fitted
                energy[pl.ds(pulsar, 1), :] = energy[pl.ds(pulsar, 1), :] + squares
                counts[pulsar] = counts[pulsar] + number
                turn_next()

            return carry

        lax.fori_loop(low, high, one_pulsar, carry)

        @pl.when(sum(rows[1:], rows[0]) == 0)
        def _():
            turn_next()

        return carry

    lax.fori_loop(0, steps, one_step, 0)
    height, core, _ = location()
    for s in range(4):
        pack(other_ref, s, 2 * ((height + s) & 3) + 1 - core, gram, fit, energy, counts)


def pack(out_ref, s, k, gram, fit, energy, counts):
    row, col = iota((128, 128), 0), iota((128, 128), 1)
    line = iota((8, 128), 0)
    spot = iota((8, 128), 1)

    @pl.when(counts[k] == 0)
    def _():
        out_ref[s] = jnp.zeros((ROWS_SENT, 128), f32)

    @pl.when(counts[k] > 0)
    def _():
        upper = gram[k, 0:128, 0:128]
        lower = gram[k, 128:256, 128:256]
        upper = 0.5 * (upper + upper.T)
        lower = 0.5 * (lower + lower.T)
        cross = 0.5 * (gram[k, 128:256, 0:128] + gram[k, 0:128, 128:256].T)
        out_ref[s, 0:128, :] = jnp.where(col > row, upper, lower)
        out_ref[s, 128:256, :] = cross
        diagonal = jnp.sum(jnp.where(col == row, upper, 0.0), axis=0, keepdims=True)
        first = jnp.sum(fit[k, 0:128, :].T, axis=0, keepdims=True)
        second = jnp.sum(fit[k, 128:256, :].T, axis=0, keepdims=True)
        power = jnp.sum(energy[pl.ds(k, 1), :], axis=1, keepdims=True)
        number = counts[k].astype(f32)
        last = jnp.where(spot == 0, power, jnp.where(spot == 1, number, 0.0))
        rest = jnp.where(line == 3, last, 0.0)
        rest = jnp.where(line == 0, diagonal, rest)
        rest = jnp.where(line == 1, first, rest)
        out_ref[s, 256:264, :] = jnp.where(line == 2, second, rest)


def keep_kernel(counts, gram, fit, energy, mine_ref):
    height, core, _ = location()
    for s in range(4):
        pack(mine_ref, s, 2 * ((height + s) & 3) + core, gram, fit, energy, counts)


def gram_parts(design, weight, residuals, slot_pulsar, slot_rows):
    slots = design.shape[0]
    piece = pltpu.VMEM((4, ROWS_SENT, 128), f32)
    smem = pl.BlockSpec(memory_space=pltpu.SMEM)
    vmem = pl.BlockSpec(memory_space=pltpu.VMEM)
    other, gram, fit, energy, counts = pl.pallas_call(
        gram_kernel,
        in_specs=[smem, smem, pl.BlockSpec(memory_space=pl.ANY), vmem, vmem],
        out_specs=[vmem, vmem, vmem, vmem, smem],
        scratch_shapes=[
            pltpu.VMEM((slots, 128, COLUMNS), jnp.bfloat16),
            pltpu.VMEM((2, COLUMNS, STEP_BLOCKS * 128), jnp.bfloat16),
            pltpu.VMEM((slots, 128), f32),
            pltpu.SemaphoreType.DMA((slots // STEP_BLOCKS,)),
        ],
        out_shape=[
            piece,
            pltpu.VMEM((GROUP_PULSARS, COLUMNS, COLUMNS), f32),
            pltpu.VMEM((GROUP_PULSARS, COLUMNS, 128), f32),
            pltpu.VMEM((GROUP_PULSARS, 128), f32),
            jax.ShapeDtypeStruct((GROUP_PULSARS,), jnp.int32),
        ],
        compiler_params=pltpu.CompilerParams(vmem_limit_bytes=24 << 20),
        name="gram",
    )(slot_pulsar, slot_rows, design, weight, residuals)
    mine = pl.pallas_call(
        keep_kernel,
        in_specs=[smem, vmem, vmem, vmem],
        out_specs=vmem,
        out_shape=piece,
        compiler_params=pltpu.CompilerParams(vmem_limit_bytes=24 << 20),
        name="keep",
    )(counts, in_vmem(gram), in_vmem(fit), in_vmem(energy))
    return mine, other


def coupling_kernel(directions_ref, out_ref, board_ref):
    _, core, _ = location()
    row, col = iota((128, 128), 0), iota((128, 128), 1)
    source = jnp.where(col < 64, 2 * col + core, 2 * col - 127 - core)
    chosen = (row == source).astype(f32)
    lines = jnp.concatenate([directions_ref[...], jnp.zeros((5, 128), f32)], axis=0)
    lines = jnp.dot(lines, chosen, precision=highest, preferred_element_type=f32)
    turned = lines.T
    cosines = jnp.zeros((128, 128), f32)
    for i in range(3):
        cosines = cosines + turned[:, i : i + 1] * lines[i : i + 1, :]
    cosines = jnp.clip(cosines, -1.0, 1.0)
    same = row == col
    spread = jnp.where(same, 1.0, 0.5 * (1.0 - cosines))
    curve = 1.5 * spread * jnp.log(spread) - 0.25 * spread + 0.5
    correlation = jnp.where(same, 1.0, curve)
    identity = jnp.where(same, 1.0, 0.0)
    tiles = [
        [correlation[8 * a : 8 * a + 8, :], identity[8 * a : 8 * a + 8, :]] for a in range(16)
    ]
    board = Board(board_ref)
    tiles, _, _, _ = eliminate_rows(tiles, 0, jnp.zeros((8, 128), f32), board, True, AHEAD)
    for a in range(16):
        out_ref[8 * a : 8 * a + 8, :] = tiles[a][1]


def coupling_inverse(directions):
    return pl.pallas_call(
        coupling_kernel,
        in_specs=[pl.BlockSpec(memory_space=pltpu.VMEM)],
        out_specs=pl.BlockSpec(memory_space=pltpu.VMEM),
        out_shape=pltpu.VMEM((128, 128), f32),
        scratch_shapes=[pltpu.VMEM((16 * 12, 8, 128), f32)],
        name="coupling",
    )(directions)


def power_column(spectrum_ref):
    inverse = 1.0 / spectrum_ref[...]
    half = iota((64, 32), 0) >> 1
    spread = jnp.where(iota((64, 32), 1) == half, jnp.broadcast_to(inverse, (64, 32)), 0.0)
    return jnp.sum(spread, axis=1, keepdims=True)


def own_kernel(
    kept,
    part0,
    part1,
    part2,
    part3,
    prior_ref,
    spectrum_ref,
    coupling_ref,
    sent_ref,
    extra_ref,
    logdet_ref,
    board_ref,
):
    row, col = iota((128, 128), 0), iota((128, 128), 1)

    def summed(lo, hi):
        near = kept[0, lo:hi, :] + part0[0, lo:hi, :]
        return (near + part1[lo:hi, :]) + (part2[lo:hi, :] + part3[lo:hi, :])

    packed = summed(0, 128)
    cross = summed(128, 256)
    rest = summed(256, 264)
    turned = packed.T
    prior = 1.0 / prior_ref[...]
    prior = jnp.concatenate([jnp.zeros((1, 64), f32), prior], axis=1)
    upper = jnp.where(col > row, packed, turned)
    upper = jnp.where(col == row, rest[0:1, :] + prior[:, 0:128], upper)
    lower = jnp.where(col <= row, packed, turned)
    lower = jnp.where(col == row, lower + prior[:, 128:256], lower)
    side = rest.T
    lane = iota((64, 128), 1)
    log_sum = jnp.zeros((8, 128), f32)

    board = Board(board_ref)

    def panel_of(parts, at, log_sum):
        tiles = [[part[8 * a : 8 * a + 8, :] for part in parts] for a in range(8)]
        _, before, after, log_sum = eliminate_rows(tiles, at, log_sum, board, False)
        old, new = [
            [jnp.concatenate([rows[a][t] for a in range(8)], axis=0) for t in range(len(parts))]
            for rows in (before, after)
        ]
        return old, new, log_sum

    def product(left, right):
        return lax.dot_general(
            left,
            right,
            (((0,), (0,)), ((), ())),
            precision=highest,
            preferred_element_type=f32,
        )

    turned_cross = cross.T
    right_top = jnp.broadcast_to(side[:, 1:2], (128, 128))
    right_low = jnp.broadcast_to(side[:, 2:3], (128, 128))
    final = jnp.where(lane < 64, upper[0:64, :], right_top[0:64, :])
    low = [jnp.where(iota((128, 128), 1) < 64, cross, right_low), lower]

    parts = [upper[64:128, :], turned_cross[64:128, :], right_top[64:128, :]]
    old, fresh, log_sum = panel_of(parts, 64, log_sum)
    quadratic = old[2] * fresh[2]
    first = jnp.where(lane < 64, fresh[0], fresh[2])
    change = product(old[1], jnp.concatenate([first, fresh[1]], axis=1))
    low = [low[0] - change[:, 0:128], low[1] - change[:, 128:256]]
    final = final - product(old[0][:, 0:64], first)

    parts = [low[0][0:64, :], low[1][0:64, :]]
    old, fresh, log_sum = panel_of(parts, 128, log_sum)
    quadratic = quadratic + old[0] * fresh[0]
    change = product(old[1][:, 64:128], jnp.concatenate(fresh, axis=1))
    final = final - product(old[0][:, 0:64], fresh[0])

    parts = [low[0][64:128, :] - change[:, 0:128], low[1][64:128, :] - change[:, 128:256]]
    old, fresh, log_sum = panel_of(parts, 192, log_sum)
    quadratic = quadratic + old[0] * fresh[0]
    final = final - product(old[0][:, 0:64], fresh[0])

    _, _, own = location()
    mine = jnp.where((row == own) & (col == own), coupling_ref[...], 0.0)
    self_coupling = total(mine)
    power = power_column(spectrum_ref)
    row64, col64 = iota((64, 128), 0), iota((64, 128), 1)
    block = final
    block = jnp.where(row64 == col64, block + self_coupling * power, block)
    block = jnp.where(col64 < 64, block, jnp.where(col64 == row64 + 64, 1.0, 0.0))
    tiles = [[block[8 * a : 8 * a + 8, :]] for a in range(8)]
    tiles, _, _, log_sum = eliminate_rows(tiles, 0, log_sum, board, True)
    solved = jnp.concatenate([tiles[a][0] for a in range(8)], axis=0)
    inverse = pltpu.roll(solved, 64, 1)
    top, bottom = inverse[0:32, :], inverse[32:64, :]
    row32, col32 = iota((32, 128), 0), iota((32, 128), 1)
    moved = pltpu.roll(bottom, 96, 1)
    triangle = jnp.where(col32 > row32, top, moved)
    folded = jnp.where(col32 < 32, triangle, top)
    lines = jnp.where(
        iota((16, 128), 1) < 64, folded[0:16, :], pltpu.roll(folded[16:32, :], 64, 1)
    )
    diagonal = jnp.sum(jnp.where(row32 == col32, top, 0.0), axis=0, keepdims=True)
    target = final
    target_line = jnp.concatenate([target, target], axis=0).T[64:65, :]
    final_line = jnp.where(iota((1, 128), 1) < 64, diagonal, target_line)
    whole = jnp.concatenate([lines, final_line], axis=0)
    whole = jnp.concatenate([whole] * 8, axis=0)
    for i in range(8):
        sent_ref[8 * LINES * i : 8 * LINES * (i + 1), :] = whole
    spent = jnp.sum(quadratic, axis=0, keepdims=True)
    left_over = rest[3:4, 0:1] - spent[:, 64:65]
    line = iota((8, 128), 0)
    extra_ref[...] = jnp.where(line == 0, left_over, rest[3:4, 1:2])
    logdet_ref[0] = log_sum[0, 0] / COLUMNS


def own_terms(parts, own_prior, spectrum, coupling):
    vmem = pl.BlockSpec(memory_space=pltpu.VMEM)
    smem = pl.BlockSpec(memory_space=pltpu.SMEM)
    return pl.pallas_call(
        own_kernel,
        in_specs=[vmem] * 8,
        out_specs=[vmem, vmem, smem],
        out_shape=[
            pltpu.VMEM((64 * LINES, 128), f32),
            pltpu.VMEM((8, 128), f32),
            jax.ShapeDtypeStruct((1,), f32),
        ],
        scratch_shapes=[pltpu.VMEM((32 * 14, 8, 128), f32)],
        name="own",
    )(*map(in_vmem, parts), own_prior, spectrum, in_vmem(coupling))


def gradient_kernel(
    near_ref,
    far_ref,
    coupling_ref,
    spectrum_ref,
    extra_ref,
    coeffs_ref,
    chi_ref,
    flat,
    inverse,
    target,
    resid,
    direction,
    mapped,
    answer,
    turned,
):
    for i in range(LINES):
        rows = pl.ds(i, 64, stride=LINES)
        both = jnp.concatenate([near_ref[rows, :], far_ref[rows, :]], axis=0).T
        for m in range(0, 128, 8):
            flat[pl.ds(m * LINES + i, 8, stride=LINES), :] = both[m : m + 8, :]
    line = iota((8, 128), 0)

    def straight_of(r, c):
        return flat[pl.ds((64 * (r // 16) + c) * LINES + r % 16, 8, stride=LINES), :]

    def crossed_of(c, r):
        at = (64 * (c // 16) + r) * LINES + c % 16
        return flat[at : at + 8, :]

    for r in range(32):
        corner = flat[r * LINES + 16 : r * LINES + 17, :]
        for c in range(0, 32, 8):
            if c > r:
                upper, lower = straight_of(r, c), crossed_of(c, r)
            elif c + 7 < r:
                upper, lower = crossed_of(c, r), straight_of(r, c)
            else:
                index = line + c
                straight, crossed = straight_of(r, c), crossed_of(c, r)
                upper = jnp.where(index > r, straight, crossed)
                upper = jnp.where(index == r, corner, upper)
                lower = jnp.where(index <= r, straight, crossed)
            inverse[r, c : c + 8, :] = upper
            inverse[32 + r, 32 + c : 40 + c, :] = lower
            inverse[r, 32 + c : 40 + c, :] = straight_of(r, 32 + c)
            inverse[32 + r, c : c + 8, :] = crossed_of(c, 32 + r)
    for c in range(0, 64, 8):
        target[c : c + 8, :] = flat[pl.ds((64 + c) * LINES + 16, 8, stride=LINES), :]

    row, col = iota((128, 128), 0), iota((128, 128), 1)
    mixing = jnp.where(row == col, 0.0, coupling_ref[...])
    power = power_column(spectrum_ref)
    resid[...] = target[...]
    direction[...] = jnp.zeros((64, 128), f32)
    mapped[...] = jnp.zeros((64, 128), f32)
    answer[...] = jnp.zeros((64, 128), f32)

    def iterate(_, carry):
        inner, curved = carry
        now = resid[...]
        sums = [jnp.zeros((8, 128), f32) for _ in range(8)]
        for k in range(64):
            line = sub_bcast(now[k // 8 * 8 : k // 8 * 8 + 8, :], k % 8)
            for c in range(8):
                sums[c] = sums[c] + inverse[k, 8 * c : 8 * c + 8, :] * line
        scaled = jnp.concatenate(sums, axis=0)
        mixed = jnp.dot(scaled, mixing, precision=highest, preferred_element_type=f32)
        image = now + power * mixed
        old_mapped = mapped[...]
        inner_next = total(now * scaled)
        straight = total(scaled * image)
        crossing = total(scaled * old_mapped)
        ratio = inner_next / inner
        curved = straight + ratio * (2.0 * crossing + ratio * curved)
        step = inner_next / curved
        toward = scaled + ratio * direction[...]
        image = image + ratio * old_mapped
        direction[...] = toward
        mapped[...] = image
        answer[...] = answer[...] + step * toward
        resid[...] = now - step * image
        return inner_next, curved

    lax.fori_loop(0, ITERS, iterate, (jnp.ones((1, 1), f32), jnp.zeros((1, 1), f32)))
    _, _, own = location()
    value = answer[...]
    gained = jnp.sum(target[...] * value, axis=0, keepdims=True)
    lane = iota((1, 128), 1)
    gained = jnp.sum(jnp.where(lane == own, gained, 0.0), axis=1, keepdims=True)
    chi = (extra_ref[0:1, 0:1] - gained) / extra_ref[1:2, 0:1]
    chi_ref[0] = chi[0, 0]
    turned[...] = jnp.concatenate([value, value], axis=0).T
    coeffs_ref[...] = turned[pl.ds(own, 1), :][:, 0:64]


def conjugate(near, far, coupling, spectrum, extra):
    vmem = pl.BlockSpec(memory_space=pltpu.VMEM)
    smem = pl.BlockSpec(memory_space=pltpu.SMEM)
    square = pltpu.VMEM((64, 128), f32)
    return pl.pallas_call(
        gradient_kernel,
        in_specs=[vmem] * 5,
        out_specs=[vmem, smem],
        out_shape=[jax.ShapeDtypeStruct((1, COMMON), f32), jax.ShapeDtypeStruct((1,), f32)],
        scratch_shapes=[
            pltpu.VMEM((WIDTH, 128), f32),
            pltpu.VMEM((64, 64, 128), f32),
            square,
            square,
            square,
            square,
            square,
            pltpu.VMEM((128, 128), f32),
        ],
        name="gradient",
    )(in_vmem(near), in_vmem(far), in_vmem(coupling), spectrum, in_vmem(extra))


def body(design, noise_weight, residuals, slot_pulsar, slot_rows, own_prior, spectrum, directions):
    count = lax.axis_size("psr") * lax.axis_size("toa")
    spectrum = spectrum.reshape(1, -1)
    mine, other = gram_parts(design, noise_weight, residuals, slot_pulsar, slot_rows)
    got = lax.ppermute(other, "toa", [(u, u ^ 1) for u in range(8)])
    parts = [mine, got]
    for s in range(1, 4):
        part = mine[s] + got[s]
        parts.append(lax.ppermute(part, "toa", [(u, (u + 2 * s) % 8) for u in range(8)]))
    coupling = coupling_inverse(directions)
    sent, extra, log_dets = own_terms(parts, own_prior, spectrum, coupling)
    groups = [list(range(c, count, 2)) for c in range(2)]
    sent = sent.reshape(64, 1, WIDTH)
    near = lax.all_to_all(sent, AXES, 0, 0, tiled=True, axis_index_groups=groups)
    near = near.reshape(64 * LINES, 128)
    far = lax.ppermute(near, "toa", [(u, u ^ 1) for u in range(8)])
    coeffs, chi_square = conjugate(near, far, coupling, spectrum, extra)
    return (coeffs, log_dets, chi_square)


def solution(mesh):
    return jax.shard_map(
        body,
        mesh=mesh,
        in_specs=(
            P(AXES, None, None),
            P(AXES, None),
            P(AXES, None),
            P(AXES),
            P(AXES),
            P(AXES, None),
            P(),
            P(),
        ),
        out_specs=(P(AXES, None), P(AXES), P(AXES)),
        check_vma=False,
    )
```

```python
import jax
import jax.numpy as jnp
from jax import lax
from jax.experimental import pallas as pl
from jax.experimental.pallas import tpu as pltpu
from jax.sharding import PartitionSpec as P


GROUP_PULSARS = 8
ITERS = 8
COLUMNS = 256
COMMON = 64
STEP_BLOCKS = 8
ROWS_SENT = 264
AHEAD = True
WIDTH = 2176
LINES = WIDTH // 128
AXES = ("psr", "toa")

highest = lax.Precision.HIGHEST
f32 = jnp.float32


def location():
    toa = lax.axis_index("toa")
    return toa >> 1, toa & 1, lax.axis_index("psr") * 4 + (toa >> 1)


def in_vmem(value):
    return pltpu.with_memory_space_constraint(value, pltpu.VMEM)


def iota(shape, dim):
    return lax.broadcasted_iota(jnp.int32, shape, dim)


def sub_bcast(value, row):
    return jnp.broadcast_to(value[row : row + 1, :], value.shape)


def lane_bcast(value, lane):
    index = jnp.full(value.shape, lane, jnp.int32)
    return jnp.take_along_axis(value, index, axis=1, mode="promise_in_bounds")


def total(value):
    return jnp.sum(jnp.sum(value, axis=0, keepdims=True), axis=1, keepdims=True)


def summed_tree(parts):
    while len(parts) > 1:
        joined = [u + v for u, v in zip(parts[::2], parts[1::2])]
        parts = joined + ([parts[-1]] if len(parts) % 2 else [])
    return parts[0]


def invert_block(cols, log_sum):
    row = iota((8, 128), 0)
    for i in range(0, 8, 2):
        first, second = row == i, row == i + 1
        c0, c1 = cols[i], cols[i + 1]
        p, q = sub_bcast(c0, i), sub_bcast(c1, i)
        r, s = sub_bcast(c0, i + 1), sub_bcast(c1, i + 1)
        det = p * s - q * r
        inverse = 1.0 / det
        log_sum = log_sum + jnp.log(det)
        for k in range(8):
            if k not in (i, i + 1):
                u, v = sub_bcast(cols[k], i), sub_bcast(cols[k], i + 1)
                n0 = s * u - q * v
                n1 = p * v - r * u
                moved = cols[k] - (c0 * n0 + c1 * n1) * inverse
                moved = jnp.where(first, n0 * inverse, moved)
                cols[k] = jnp.where(second, n1 * inverse, moved)
        left = jnp.where(first, s, jnp.where(second, -r, c1 * r - c0 * s))
        right = jnp.where(first, -q, jnp.where(second, p, c0 * q - c1 * p))
        cols[i] = left * inverse
        cols[i + 1] = right * inverse
    return cols, log_sum


class Board:
    def __init__(self, ref):
        self.ref, self.used = ref, 0

    def rows(self, value):
        at = self.used
        self.used = at + 1
        self.ref[at] = value
        return [self.ref[at, k : k + 1, :] for k in range(8)]


def eliminate_rows(tiles, first_lane, log_sum, board, whole, ahead=True):
    count = len(tiles)
    width = len(tiles[0])
    before, after = [], []

    def columns(a, b):
        at = first_lane + 8 * b
        return [lane_bcast(tiles[a][at // 128], at % 128 + k) for k in range(8)]

    cols = columns(0, 0)
    for b in range(count):
        cols, log_sum = invert_block(cols, log_sum)
        last = b + 1 == count
        factors = {}
        if not last and ahead:
            factor = columns(b + 1, b)
            factors[b + 1] = factor
            coming = columns(b + 1, b + 1)
            spots = [board.rows(value) for value in factor]
            for j in range(8):
                solved = summed_tree([cols[m] * spots[m][j] for m in range(8)])
                change = summed_tree([factor[k] * sub_bcast(solved, k) for k in range(8)])
                coming[j] = coming[j] - change
        fresh, spread = [], []
        for t in range(width):
            rows = board.rows(tiles[b][t])
            fresh.append(summed_tree([cols[k] * rows[k] for k in range(8)]))
            spread.append(board.rows(fresh[t]))
        before.append(tiles[b])
        after.append(fresh)
        for a in range(0 if whole else b + 1, count):
            if a != b:
                factor = factors[a] if a in factors else columns(a, b)
                tiles[a] = [
                    tiles[a][t] - summed_tree([factor[k] * spread[t][k] for k in range(8)])
                    for t in range(width)
                ]
        if whole:
            tiles[b] = fresh
        if not last:
            cols = coming if ahead else columns(b + 1, b + 1)
    return tiles, before, after, log_sum


def gram_kernel(
    pulsar_ref,
    rows_ref,
    design_ref,
    weight_ref,
    resid_ref,
    mine_ref,
    other_ref,
    blocks,
    gram,
    fit,
    energy,
    wide_resid,
    counts,
    arrived,
):
    slots = weight_ref.shape[0]
    steps = slots // STEP_BLOCKS

    def load(step):
        where = pl.ds(step * STEP_BLOCKS, STEP_BLOCKS)
        return pltpu.make_async_copy(design_ref.at[where], blocks.at[where], arrived.at[step])

    for step in range(steps):
        load(step).start()
    gram[...] = jnp.zeros(gram.shape, f32)
    fit[...] = jnp.zeros(fit.shape, f32)
    energy[...] = jnp.zeros(energy.shape, f32)
    for k in range(GROUP_PULSARS):
        counts[k] = 0
    wide_resid[...] = resid_ref[...].astype(f32)
    lane = iota((1, 128), 1)

    def one_step(step, carry):
        load(step).wait()
        at = step * STEP_BLOCKS
        pulsars = [pulsar_ref[at + i] for i in range(STEP_BLOCKS)]
        rows = [rows_ref[at + i] for i in range(STEP_BLOCKS)]
        same = pulsars[1] == pulsars[0]
        for i in range(2, STEP_BLOCKS):
            same = same & (pulsars[i] == pulsars[0])
        low = jnp.where(same, pulsars[0], 0)
        high = jnp.where(same, pulsars[0] + 1, GROUP_PULSARS)

        def one_pulsar(pulsar, carry):
            valid = [jnp.where(pulsars[i] == pulsar, rows[i], 0) for i in range(STEP_BLOCKS)]
            number = valid[0]
            for i in range(1, STEP_BLOCKS):
                number = number + valid[i]

            @pl.when(number > 0)
            def _():
                pieces, fitted, squares = [], None, None
                for i in range(STEP_BLOCKS):
                    weight = jnp.where(lane < valid[i], weight_ref[pl.ds(at + i, 1), :], 0.0)
                    resid = wide_resid[pl.ds(at + i, 1), :]
                    turned = blocks[at + i].T.astype(f32)
                    weighted = (turned * weight).astype(jnp.bfloat16)
                    pieces.append(weighted)
                    product = weighted.astype(f32) * resid
                    square = weight * resid * resid
                    fitted = product if fitted is None else fitted + product
                    squares = square if squares is None else squares + square
                left = jnp.concatenate(pieces, axis=1)
                right = blocks[pl.ds(at, STEP_BLOCKS)].reshape(STEP_BLOCKS * 128, COLUMNS)
                gram[pulsar] = gram[pulsar] + jnp.dot(left, right, preferred_element_type=f32)
                fit[pulsar] = fit[pulsar] + fitted
                energy[pl.ds(pulsar, 1), :] = energy[pl.ds(pulsar, 1), :] + squares
                counts[pulsar] = counts[pulsar] + number

            return carry

        return lax.fori_loop(low, high, one_pulsar, carry)

    lax.fori_loop(0, steps, one_step, 0)

    row, col = iota((128, 128), 0), iota((128, 128), 1)
    line = iota((8, 128), 0)
    spot = iota((8, 128), 1)
    height, core, _ = location()

    def pack(out_ref, s, k):
        @pl.when(counts[k] == 0)
        def _():
            out_ref[s] = jnp.zeros((ROWS_SENT, 128), f32)

        @pl.when(counts[k] > 0)
        def _():
            upper = gram[k, 0:128, 0:128]
            lower = gram[k, 128:256, 128:256]
            upper = 0.5 * (upper + upper.T)
            lower = 0.5 * (lower + lower.T)
            cross = 0.5 * (gram[k, 128:256, 0:128] + gram[k, 0:128, 128:256].T)
            out_ref[s, 0:128, :] = jnp.where(col > row, upper, lower)
            out_ref[s, 128:256, :] = cross
            diagonal = jnp.sum(jnp.where(col == row, upper, 0.0), axis=0, keepdims=True)
            first = jnp.sum(fit[k, 0:128, :].T, axis=0, keepdims=True)
            second = jnp.sum(fit[k, 128:256, :].T, axis=0, keepdims=True)
            power = jnp.sum(energy[pl.ds(k, 1), :], axis=1, keepdims=True)
            number = counts[k].astype(f32)
            last = jnp.where(spot == 0, power, jnp.where(spot == 1, number, 0.0))
            rest = jnp.where(line == 3, last, 0.0)
            rest = jnp.where(line == 0, diagonal, rest)
            rest = jnp.where(line == 1, first, rest)
            out_ref[s, 256:264, :] = jnp.where(line == 2, second, rest)

    for s in range(4):
        base = 2 * ((height + s) & 3)
        pack(other_ref, s, base + 1 - core)
        pack(mine_ref, s, base + core)


def gram_parts(design, weight, residuals, slot_pulsar, slot_rows):
    slots = design.shape[0]
    piece = pltpu.VMEM((4, ROWS_SENT, 128), f32)
    smem = pl.BlockSpec(memory_space=pltpu.SMEM)
    vmem = pl.BlockSpec(memory_space=pltpu.VMEM)
    hbm = pl.BlockSpec(memory_space=pl.ANY)
    return pl.pallas_call(
        gram_kernel,
        in_specs=[smem, smem, hbm, vmem, vmem],
        out_specs=[vmem, vmem],
        scratch_shapes=[
            pltpu.VMEM((slots, 128, COLUMNS), jnp.bfloat16),
            pltpu.VMEM((GROUP_PULSARS, COLUMNS, COLUMNS), f32),
            pltpu.VMEM((GROUP_PULSARS, COLUMNS, 128), f32),
            pltpu.VMEM((GROUP_PULSARS, 128), f32),
            pltpu.VMEM((slots, 128), f32),
            pltpu.SMEM((GROUP_PULSARS,), jnp.int32),
            pltpu.SemaphoreType.DMA((slots // STEP_BLOCKS,)),
        ],
        out_shape=[piece, piece],
        name="gram",
    )(slot_pulsar, slot_rows, design, weight, residuals)


def coupling_kernel(directions_ref, out_ref, board_ref):
    _, core, _ = location()
    row, col = iota((128, 128), 0), iota((128, 128), 1)
    source = jnp.where(col < 64, 2 * col + core, 2 * col - 127 - core)
    chosen = (row == source).astype(f32)
    lines = jnp.concatenate([directions_ref[...], jnp.zeros((5, 128), f32)], axis=0)
    lines = jnp.dot(lines, chosen, precision=highest, preferred_element_type=f32)
    turned = lines.T
    cosines = jnp.zeros((128, 128), f32)
    for i in range(3):
        cosines = cosines + turned[:, i : i + 1] * lines[i : i + 1, :]
    cosines = jnp.clip(cosines, -1.0, 1.0)
    same = row == col
    spread = jnp.where(same, 1.0, 0.5 * (1.0 - cosines))
    curve = 1.5 * spread * jnp.log(spread) - 0.25 * spread + 0.5
    correlation = jnp.where(same, 1.0, curve)
    identity = jnp.where(same, 1.0, 0.0)
    tiles = [
        [correlation[8 * a : 8 * a + 8, :], identity[8 * a : 8 * a + 8, :]] for a in range(16)
    ]
    board = Board(board_ref)
    tiles, _, _, _ = eliminate_rows(tiles, 0, jnp.zeros((8, 128), f32), board, True, AHEAD)
    for a in range(16):
        out_ref[8 * a : 8 * a + 8, :] = tiles[a][1]


def coupling_inverse(directions):
    return pl.pallas_call(
        coupling_kernel,
        in_specs=[pl.BlockSpec(memory_space=pltpu.VMEM)],
        out_specs=pl.BlockSpec(memory_space=pltpu.VMEM),
        out_shape=pltpu.VMEM((128, 128), f32),
        scratch_shapes=[pltpu.VMEM((16 * 12, 8, 128), f32)],
        name="coupling",
    )(directions)


def power_column(spectrum_ref):
    inverse = 1.0 / spectrum_ref[...]
    half = iota((64, 32), 0) >> 1
    spread = jnp.where(iota((64, 32), 1) == half, jnp.broadcast_to(inverse, (64, 32)), 0.0)
    return jnp.sum(spread, axis=1, keepdims=True)


def own_kernel(
    kept,
    part0,
    part1,
    part2,
    part3,
    prior_ref,
    spectrum_ref,
    coupling_ref,
    sent_ref,
    extra_ref,
    logdet_ref,
    board_ref,
):
    row, col = iota((128, 128), 0), iota((128, 128), 1)

    def summed(lo, hi):
        near = kept[0, lo:hi, :] + part0[0, lo:hi, :]
        return (near + part1[lo:hi, :]) + (part2[lo:hi, :] + part3[lo:hi, :])

    packed = summed(0, 128)
    cross = summed(128, 256)
    rest = summed(256, 264)
    turned = packed.T
    prior = 1.0 / prior_ref[...]
    prior = jnp.concatenate([jnp.zeros((1, 64), f32), prior], axis=1)
    upper = jnp.where(col > row, packed, turned)
    upper = jnp.where(col == row, rest[0:1, :] + prior[:, 0:128], upper)
    lower = jnp.where(col <= row, packed, turned)
    lower = jnp.where(col == row, lower + prior[:, 128:256], lower)
    side = rest.T
    lane = iota((64, 128), 1)
    log_sum = jnp.zeros((8, 128), f32)

    board = Board(board_ref)

    def panel_of(parts, at, log_sum):
        tiles = [[part[8 * a : 8 * a + 8, :] for part in parts] for a in range(8)]
        _, before, after, log_sum = eliminate_rows(tiles, at, log_sum, board, False)
        old, new = [
            [jnp.concatenate([rows[a][t] for a in range(8)], axis=0) for t in range(len(parts))]
            for rows in (before, after)
        ]
        return old, new, log_sum

    def product(left, right):
        return lax.dot_general(
            left,
            right,
            (((0,), (0,)), ((), ())),
            precision=highest,
            preferred_element_type=f32,
        )

    turned_cross = cross.T
    right_top = jnp.broadcast_to(side[:, 1:2], (128, 128))
    right_low = jnp.broadcast_to(side[:, 2:3], (128, 128))
    final = jnp.where(lane < 64, upper[0:64, :], right_top[0:64, :])
    low = [jnp.where(iota((128, 128), 1) < 64, cross, right_low), lower]

    parts = [upper[64:128, :], turned_cross[64:128, :], right_top[64:128, :]]
    old, fresh, log_sum = panel_of(parts, 64, log_sum)
    quadratic = old[2] * fresh[2]
    first = jnp.where(lane < 64, fresh[0], fresh[2])
    change = product(old[1], jnp.concatenate([first, fresh[1]], axis=1))
    low = [low[0] - change[:, 0:128], low[1] - change[:, 128:256]]
    final = final - product(old[0][:, 0:64], first)

    parts = [low[0][0:64, :], low[1][0:64, :]]
    old, fresh, log_sum = panel_of(parts, 128, log_sum)
    quadratic = quadratic + old[0] * fresh[0]
    change = product(old[1][:, 64:128], jnp.concatenate(fresh, axis=1))
    final = final - product(old[0][:, 0:64], fresh[0])

    parts = [low[0][64:128, :] - change[:, 0:128], low[1][64:128, :] - change[:, 128:256]]
    old, fresh, log_sum = panel_of(parts, 192, log_sum)
    quadratic = quadratic + old[0] * fresh[0]
    final = final - product(old[0][:, 0:64], fresh[0])

    _, _, own = location()
    mine = jnp.where((row == own) & (col == own), coupling_ref[...], 0.0)
    self_coupling = total(mine)
    power = power_column(spectrum_ref)
    row64, col64 = iota((64, 128), 0), iota((64, 128), 1)
    block = final
    block = jnp.where(row64 == col64, block + self_coupling * power, block)
    block = jnp.where(col64 < 64, block, jnp.where(col64 == row64 + 64, 1.0, 0.0))
    tiles = [[block[8 * a : 8 * a + 8, :]] for a in range(8)]
    tiles, _, _, log_sum = eliminate_rows(tiles, 0, log_sum, board, True)
    solved = jnp.concatenate([tiles[a][0] for a in range(8)], axis=0)
    inverse = pltpu.roll(solved, 64, 1)
    top, bottom = inverse[0:32, :], inverse[32:64, :]
    row32, col32 = iota((32, 128), 0), iota((32, 128), 1)
    moved = pltpu.roll(bottom, 96, 1)
    triangle = jnp.where(col32 > row32, top, moved)
    folded = jnp.where(col32 < 32, triangle, top)
    lines = jnp.where(
        iota((16, 128), 1) < 64, folded[0:16, :], pltpu.roll(folded[16:32, :], 64, 1)
    )
    diagonal = jnp.sum(jnp.where(row32 == col32, top, 0.0), axis=0, keepdims=True)
    target = final
    target_line = jnp.concatenate([target, target], axis=0).T[64:65, :]
    final_line = jnp.where(iota((1, 128), 1) < 64, diagonal, target_line)
    whole = jnp.concatenate([lines, final_line], axis=0)
    whole = jnp.concatenate([whole] * 8, axis=0)
    for i in range(8):
        sent_ref[8 * LINES * i : 8 * LINES * (i + 1), :] = whole
    spent = jnp.sum(quadratic, axis=0, keepdims=True)
    left_over = rest[3:4, 0:1] - spent[:, 64:65]
    line = iota((8, 128), 0)
    extra_ref[...] = jnp.where(line == 0, left_over, rest[3:4, 1:2])
    logdet_ref[0] = log_sum[0, 0] / COLUMNS


def own_terms(parts, own_prior, spectrum, coupling):
    vmem = pl.BlockSpec(memory_space=pltpu.VMEM)
    smem = pl.BlockSpec(memory_space=pltpu.SMEM)
    return pl.pallas_call(
        own_kernel,
        in_specs=[vmem] * 8,
        out_specs=[vmem, vmem, smem],
        out_shape=[
            pltpu.VMEM((64 * LINES, 128), f32),
            pltpu.VMEM((8, 128), f32),
            jax.ShapeDtypeStruct((1,), f32),
        ],
        scratch_shapes=[pltpu.VMEM((32 * 14, 8, 128), f32)],
        name="own",
    )(*map(in_vmem, parts), own_prior, spectrum, in_vmem(coupling))


def gradient_kernel(
    near_ref,
    far_ref,
    coupling_ref,
    spectrum_ref,
    extra_ref,
    coeffs_ref,
    chi_ref,
    flat,
    inverse,
    target,
    resid,
    direction,
    mapped,
    answer,
    turned,
):
    for i in range(LINES):
        rows = pl.ds(i, 64, stride=LINES)
        both = jnp.concatenate([near_ref[rows, :], far_ref[rows, :]], axis=0).T
        for m in range(0, 128, 8):
            flat[pl.ds(m * LINES + i, 8, stride=LINES), :] = both[m : m + 8, :]
    line = iota((8, 128), 0)

    def straight_of(r, c):
        return flat[pl.ds((64 * (r // 16) + c) * LINES + r % 16, 8, stride=LINES), :]

    def crossed_of(c, r):
        at = (64 * (c // 16) + r) * LINES + c % 16
        return flat[at : at + 8, :]

    for r in range(32):
        corner = flat[r * LINES + 16 : r * LINES + 17, :]
        for c in range(0, 32, 8):
            if c > r:
                upper, lower = straight_of(r, c), crossed_of(c, r)
            elif c + 7 < r:
                upper, lower = crossed_of(c, r), straight_of(r, c)
            else:
                index = line + c
                straight, crossed = straight_of(r, c), crossed_of(c, r)
                upper = jnp.where(index > r, straight, crossed)
                upper = jnp.where(index == r, corner, upper)
                lower = jnp.where(index <= r, straight, crossed)
            inverse[r, c : c + 8, :] = upper
            inverse[32 + r, 32 + c : 40 + c, :] = lower
            inverse[r, 32 + c : 40 + c, :] = straight_of(r, 32 + c)
            inverse[32 + r, c : c + 8, :] = crossed_of(c, 32 + r)
    for c in range(0, 64, 8):
        target[c : c + 8, :] = flat[pl.ds((64 + c) * LINES + 16, 8, stride=LINES), :]

    row, col = iota((128, 128), 0), iota((128, 128), 1)
    mixing = jnp.where(row == col, 0.0, coupling_ref[...])
    power = power_column(spectrum_ref)
    resid[...] = target[...]
    direction[...] = jnp.zeros((64, 128), f32)
    mapped[...] = jnp.zeros((64, 128), f32)
    answer[...] = jnp.zeros((64, 128), f32)

    def iterate(_, carry):
        inner, curved = carry
        now = resid[...]
        sums = [jnp.zeros((8, 128), f32) for _ in range(8)]
        for k in range(64):
            line = sub_bcast(now[k // 8 * 8 : k // 8 * 8 + 8, :], k % 8)
            for c in range(8):
                sums[c] = sums[c] + inverse[k, 8 * c : 8 * c + 8, :] * line
        scaled = jnp.concatenate(sums, axis=0)
        mixed = jnp.dot(scaled, mixing, precision=highest, preferred_element_type=f32)
        image = now + power * mixed
        old_mapped = mapped[...]
        inner_next = total(now * scaled)
        straight = total(scaled * image)
        crossing = total(scaled * old_mapped)
        ratio = inner_next / inner
        curved = straight + ratio * (2.0 * crossing + ratio * curved)
        step = inner_next / curved
        toward = scaled + ratio * direction[...]
        image = image + ratio * old_mapped
        direction[...] = toward
        mapped[...] = image
        answer[...] = answer[...] + step * toward
        resid[...] = now - step * image
        return inner_next, curved

    lax.fori_loop(0, ITERS, iterate, (jnp.ones((1, 1), f32), jnp.zeros((1, 1), f32)))
    _, _, own = location()
    value = answer[...]
    gained = jnp.sum(target[...] * value, axis=0, keepdims=True)
    lane = iota((1, 128), 1)
    gained = jnp.sum(jnp.where(lane == own, gained, 0.0), axis=1, keepdims=True)
    chi = (extra_ref[0:1, 0:1] - gained) / extra_ref[1:2, 0:1]
    chi_ref[0] = chi[0, 0]
    turned[...] = jnp.concatenate([value, value], axis=0).T
    coeffs_ref[...] = turned[pl.ds(own, 1), :][:, 0:64]


def conjugate(near, far, coupling, spectrum, extra):
    vmem = pl.BlockSpec(memory_space=pltpu.VMEM)
    smem = pl.BlockSpec(memory_space=pltpu.SMEM)
    square = pltpu.VMEM((64, 128), f32)
    return pl.pallas_call(
        gradient_kernel,
        in_specs=[vmem] * 5,
        out_specs=[vmem, smem],
        out_shape=[jax.ShapeDtypeStruct((1, COMMON), f32), jax.ShapeDtypeStruct((1,), f32)],
        scratch_shapes=[
            pltpu.VMEM((WIDTH, 128), f32),
            pltpu.VMEM((64, 64, 128), f32),
            square,
            square,
            square,
            square,
            square,
            pltpu.VMEM((128, 128), f32),
        ],
        name="gradient",
    )(in_vmem(near), in_vmem(far), in_vmem(coupling), spectrum, in_vmem(extra))


def body(design, noise_weight, residuals, slot_pulsar, slot_rows, own_prior, spectrum, directions):
    count = lax.axis_size("psr") * lax.axis_size("toa")
    spectrum = spectrum.reshape(1, -1)
    mine, other = gram_parts(design, noise_weight, residuals, slot_pulsar, slot_rows)
    got = lax.ppermute(other, "toa", [(u, u ^ 1) for u in range(8)])
    parts = [mine, got]
    for s in range(1, 4):
        part = mine[s] + got[s]
        parts.append(lax.ppermute(part, "toa", [(u, (u + 2 * s) % 8) for u in range(8)]))
    coupling = coupling_inverse(directions)
    sent, extra, log_dets = own_terms(parts, own_prior, spectrum, coupling)
    groups = [list(range(c, count, 2)) for c in range(2)]
    sent = sent.reshape(64, 1, WIDTH)
    near = lax.all_to_all(sent, AXES, 0, 0, tiled=True, axis_index_groups=groups)
    near = near.reshape(64 * LINES, 128)
    far = lax.ppermute(near, "toa", [(u, u ^ 1) for u in range(8)])
    coeffs, chi_square = conjugate(near, far, coupling, spectrum, extra)
    return (coeffs, log_dets, chi_square)


def solution(mesh):
    return jax.shard_map(
        body,
        mesh=mesh,
        in_specs=(
            P(AXES, None, None),
            P(AXES, None),
            P(AXES, None),
            P(AXES),
            P(AXES),
            P(AXES, None),
            P(),
            P(),
        ),
        out_specs=(P(AXES, None), P(AXES), P(AXES)),
        check_vma=False,
    )
```

```python
import jax
import jax.numpy as jnp
from jax import lax
from jax.experimental import pallas as pl
from jax.experimental.pallas import tpu as pltpu
from jax.sharding import PartitionSpec as P


GROUP_PULSARS = 8
ITERS = 8
COLUMNS = 256
COMMON = 64
STEP_BLOCKS = 8
ROWS_SENT = 264
AHEAD = True
WIDTH = 2176
LINES = WIDTH // 128
AXES = ("psr", "toa")

highest = lax.Precision.HIGHEST
f32 = jnp.float32


def location():
    toa = lax.axis_index("toa")
    return toa >> 1, toa & 1, lax.axis_index("psr") * 4 + (toa >> 1)


def in_vmem(value):
    return pltpu.with_memory_space_constraint(value, pltpu.VMEM)


def iota(shape, dim):
    return lax.broadcasted_iota(jnp.int32, shape, dim)


def sub_bcast(value, row):
    return jnp.broadcast_to(value[row : row + 1, :], value.shape)


def lane_bcast(value, lane):
    index = jnp.full(value.shape, lane, jnp.int32)
    return jnp.take_along_axis(value, index, axis=1, mode="promise_in_bounds")


def total(value):
    return jnp.sum(jnp.sum(value, axis=0, keepdims=True), axis=1, keepdims=True)


def summed_tree(parts):
    while len(parts) > 1:
        joined = [u + v for u, v in zip(parts[::2], parts[1::2])]
        parts = joined + ([parts[-1]] if len(parts) % 2 else [])
    return parts[0]


def invert_block(cols, log_sum):
    row = iota((8, 128), 0)
    for i in range(0, 8, 2):
        first, second = row == i, row == i + 1
        c0, c1 = cols[i], cols[i + 1]
        p, q = sub_bcast(c0, i), sub_bcast(c1, i)
        r, s = sub_bcast(c0, i + 1), sub_bcast(c1, i + 1)
        det = p * s - q * r
        inverse = 1.0 / det
        log_sum = log_sum + jnp.log(det)
        for k in range(8):
            if k not in (i, i + 1):
                u, v = sub_bcast(cols[k], i), sub_bcast(cols[k], i + 1)
                n0 = s * u - q * v
                n1 = p * v - r * u
                moved = cols[k] - (c0 * n0 + c1 * n1) * inverse
                moved = jnp.where(first, n0 * inverse, moved)
                cols[k] = jnp.where(second, n1 * inverse, moved)
        left = jnp.where(first, s, jnp.where(second, -r, c1 * r - c0 * s))
        right = jnp.where(first, -q, jnp.where(second, p, c0 * q - c1 * p))
        cols[i] = left * inverse
        cols[i + 1] = right * inverse
    return cols, log_sum


class Board:
    def __init__(self, ref):
        self.ref, self.used = ref, 0

    def rows(self, value):
        at = self.used
        self.used = at + 1
        self.ref[at] = value
        return [self.ref[at, k : k + 1, :] for k in range(8)]


def eliminate_rows(tiles, first_lane, log_sum, board, whole, ahead=True):
    count = len(tiles)
    width = len(tiles[0])
    before, after = [], []

    def columns(a, b):
        at = first_lane + 8 * b
        return [lane_bcast(tiles[a][at // 128], at % 128 + k) for k in range(8)]

    cols = columns(0, 0)
    for b in range(count):
        cols, log_sum = invert_block(cols, log_sum)
        last = b + 1 == count
        factors = {}
        if not last and ahead:
            factor = columns(b + 1, b)
            factors[b + 1] = factor
            coming = columns(b + 1, b + 1)
            spots = [board.rows(value) for value in factor]
            for j in range(8):
                solved = summed_tree([cols[m] * spots[m][j] for m in range(8)])
                change = summed_tree([factor[k] * sub_bcast(solved, k) for k in range(8)])
                coming[j] = coming[j] - change
        fresh, spread = [], []
        for t in range(width):
            rows = board.rows(tiles[b][t])
            fresh.append(summed_tree([cols[k] * rows[k] for k in range(8)]))
            spread.append(board.rows(fresh[t]))
        before.append(tiles[b])
        after.append(fresh)
        for a in range(0 if whole else b + 1, count):
            if a != b:
                factor = factors[a] if a in factors else columns(a, b)
                tiles[a] = [
                    tiles[a][t] - summed_tree([factor[k] * spread[t][k] for k in range(8)])
                    for t in range(width)
                ]
        if whole:
            tiles[b] = fresh
        if not last:
            cols = coming if ahead else columns(b + 1, b + 1)
    return tiles, before, after, log_sum


def gram_kernel(
    pulsar_ref,
    rows_ref,
    design_ref,
    weight_ref,
    resid_ref,
    mine_ref,
    other_ref,
    blocks,
    gram,
    fit,
    energy,
    wide_resid,
    counts,
    arrived,
):
    slots = weight_ref.shape[0]
    steps = slots // STEP_BLOCKS

    def load(step):
        where = pl.ds(step * STEP_BLOCKS, STEP_BLOCKS)
        return pltpu.make_async_copy(design_ref.at[where], blocks.at[where], arrived.at[step])

    for step in range(steps):
        load(step).start()
    gram[...] = jnp.zeros(gram.shape, f32)
    fit[...] = jnp.zeros(fit.shape, f32)
    energy[...] = jnp.zeros(energy.shape, f32)
    for k in range(GROUP_PULSARS):
        counts[k] = 0
    wide_resid[...] = resid_ref[...].astype(f32)
    lane = iota((1, 128), 1)

    def one_step(step, carry):
        load(step).wait()
        at = step * STEP_BLOCKS
        pulsars = [pulsar_ref[at + i] for i in range(STEP_BLOCKS)]
        rows = [rows_ref[at + i] for i in range(STEP_BLOCKS)]
        same = pulsars[1] == pulsars[0]
        for i in range(2, STEP_BLOCKS):
            same = same & (pulsars[i] == pulsars[0])
        low = jnp.where(same, pulsars[0], 0)
        high = jnp.where(same, pulsars[0] + 1, GROUP_PULSARS)

        def one_pulsar(pulsar, carry):
            valid = [jnp.where(pulsars[i] == pulsar, rows[i], 0) for i in range(STEP_BLOCKS)]
            number = valid[0]
            for i in range(1, STEP_BLOCKS):
                number = number + valid[i]

            @pl.when(number > 0)
            def _():
                pieces, fitted, squares = [], None, None
                for i in range(STEP_BLOCKS):
                    weight = jnp.where(lane < valid[i], weight_ref[pl.ds(at + i, 1), :], 0.0)
                    resid = wide_resid[pl.ds(at + i, 1), :]
                    turned = blocks[at + i].T.astype(f32)
                    weighted = (turned * weight).astype(jnp.bfloat16)
                    pieces.append(weighted)
                    product = weighted.astype(f32) * resid
                    square = weight * resid * resid
                    fitted = product if fitted is None else fitted + product
                    squares = square if squares is None else squares + square
                left = jnp.concatenate(pieces, axis=1)
                right = blocks[pl.ds(at, STEP_BLOCKS)].reshape(STEP_BLOCKS * 128, COLUMNS)
                gram[pulsar] = gram[pulsar] + jnp.dot(left, right, preferred_element_type=f32)
                fit[pulsar] = fit[pulsar] + fitted
                energy[pl.ds(pulsar, 1), :] = energy[pl.ds(pulsar, 1), :] + squares
                counts[pulsar] = counts[pulsar] + number

            return carry

        return lax.fori_loop(low, high, one_pulsar, carry)

    lax.fori_loop(0, steps, one_step, 0)

    row, col = iota((128, 128), 0), iota((128, 128), 1)
    line = iota((8, 128), 0)
    spot = iota((8, 128), 1)
    height, core, _ = location()

    def pack(out_ref, s, k):
        @pl.when(counts[k] == 0)
        def _():
            out_ref[s] = jnp.zeros((ROWS_SENT, 128), f32)

        @pl.when(counts[k] > 0)
        def _():
            upper = gram[k, 0:128, 0:128]
            lower = gram[k, 128:256, 128:256]
            upper = 0.5 * (upper + upper.T)
            lower = 0.5 * (lower + lower.T)
            cross = 0.5 * (gram[k, 128:256, 0:128] + gram[k, 0:128, 128:256].T)
            out_ref[s, 0:128, :] = jnp.where(col > row, upper, lower)
            out_ref[s, 128:256, :] = cross
            diagonal = jnp.sum(jnp.where(col == row, upper, 0.0), axis=0, keepdims=True)
            first = jnp.sum(fit[k, 0:128, :].T, axis=0, keepdims=True)
            second = jnp.sum(fit[k, 128:256, :].T, axis=0, keepdims=True)
            power = jnp.sum(energy[pl.ds(k, 1), :], axis=1, keepdims=True)
            number = counts[k].astype(f32)
            last = jnp.where(spot == 0, power, jnp.where(spot == 1, number, 0.0))
            rest = jnp.where(line == 3, last, 0.0)
            rest = jnp.where(line == 0, diagonal, rest)
            rest = jnp.where(line == 1, first, rest)
            out_ref[s, 256:264, :] = jnp.where(line == 2, second, rest)

    for s in range(4):
        base = 2 * ((height + s) & 3)
        pack(other_ref, s, base + 1 - core)
        pack(mine_ref, s, base + core)


def gram_parts(design, weight, residuals, slot_pulsar, slot_rows):
    slots = design.shape[0]
    piece = pltpu.VMEM((4, ROWS_SENT, 128), f32)
    smem = pl.BlockSpec(memory_space=pltpu.SMEM)
    vmem = pl.BlockSpec(memory_space=pltpu.VMEM)
    hbm = pl.BlockSpec(memory_space=pl.ANY)
    return pl.pallas_call(
        gram_kernel,
        in_specs=[smem, smem, hbm, vmem, vmem],
        out_specs=[vmem, vmem],
        scratch_shapes=[
            pltpu.VMEM((slots, 128, COLUMNS), jnp.bfloat16),
            pltpu.VMEM((GROUP_PULSARS, COLUMNS, COLUMNS), f32),
            pltpu.VMEM((GROUP_PULSARS, COLUMNS, 128), f32),
            pltpu.VMEM((GROUP_PULSARS, 128), f32),
            pltpu.VMEM((slots, 128), f32),
            pltpu.SMEM((GROUP_PULSARS,), jnp.int32),
            pltpu.SemaphoreType.DMA((slots // STEP_BLOCKS,)),
        ],
        out_shape=[piece, piece],
        name="gram",
    )(slot_pulsar, slot_rows, design, weight, residuals)


def coupling_kernel(directions_ref, out_ref, board_ref):
    _, core, _ = location()
    row, col = iota((128, 128), 0), iota((128, 128), 1)
    source = jnp.where(col < 64, 2 * col + core, 2 * col - 127 - core)
    chosen = (row == source).astype(f32)
    lines = jnp.concatenate([directions_ref[...], jnp.zeros((5, 128), f32)], axis=0)
    lines = jnp.dot(lines, chosen, precision=highest, preferred_element_type=f32)
    turned = lines.T
    cosines = jnp.zeros((128, 128), f32)
    for i in range(3):
        cosines = cosines + turned[:, i : i + 1] * lines[i : i + 1, :]
    cosines = jnp.clip(cosines, -1.0, 1.0)
    same = row == col
    spread = jnp.where(same, 1.0, 0.5 * (1.0 - cosines))
    curve = 1.5 * spread * jnp.log(spread) - 0.25 * spread + 0.5
    correlation = jnp.where(same, 1.0, curve)
    identity = jnp.where(same, 1.0, 0.0)
    tiles = [
        [correlation[8 * a : 8 * a + 8, :], identity[8 * a : 8 * a + 8, :]] for a in range(16)
    ]
    board = Board(board_ref)
    tiles, _, _, _ = eliminate_rows(tiles, 0, jnp.zeros((8, 128), f32), board, True, AHEAD)
    for a in range(16):
        out_ref[8 * a : 8 * a + 8, :] = tiles[a][1]


def coupling_inverse(directions):
    return pl.pallas_call(
        coupling_kernel,
        in_specs=[pl.BlockSpec(memory_space=pltpu.VMEM)],
        out_specs=pl.BlockSpec(memory_space=pltpu.VMEM),
        out_shape=pltpu.VMEM((128, 128), f32),
        scratch_shapes=[pltpu.VMEM((16 * 12, 8, 128), f32)],
        name="coupling",
    )(directions)


def power_column(spectrum_ref):
    inverse = 1.0 / spectrum_ref[...]
    half = iota((64, 32), 0) >> 1
    spread = jnp.where(iota((64, 32), 1) == half, jnp.broadcast_to(inverse, (64, 32)), 0.0)
    return jnp.sum(spread, axis=1, keepdims=True)


def own_kernel(
    kept,
    part0,
    part1,
    part2,
    part3,
    prior_ref,
    spectrum_ref,
    coupling_ref,
    sent_ref,
    extra_ref,
    logdet_ref,
    board_ref,
):
    row, col = iota((128, 128), 0), iota((128, 128), 1)

    def summed(lo, hi):
        near = kept[0, lo:hi, :] + part0[0, lo:hi, :]
        return (near + part1[lo:hi, :]) + (part2[lo:hi, :] + part3[lo:hi, :])

    packed = summed(0, 128)
    cross = summed(128, 256)
    rest = summed(256, 264)
    turned = packed.T
    prior = 1.0 / prior_ref[...]
    prior = jnp.concatenate([jnp.zeros((1, 64), f32), prior], axis=1)
    upper = jnp.where(col > row, packed, turned)
    upper = jnp.where(col == row, rest[0:1, :] + prior[:, 0:128], upper)
    lower = jnp.where(col <= row, packed, turned)
    lower = jnp.where(col == row, lower + prior[:, 128:256], lower)
    side = rest.T
    lane = iota((64, 128), 1)
    log_sum = jnp.zeros((8, 128), f32)

    board = Board(board_ref)

    def panel_of(parts, at, log_sum):
        tiles = [[part[8 * a : 8 * a + 8, :] for part in parts] for a in range(8)]
        _, before, after, log_sum = eliminate_rows(tiles, at, log_sum, board, False)
        old, new = [
            [jnp.concatenate([rows[a][t] for a in range(8)], axis=0) for t in range(len(parts))]
            for rows in (before, after)
        ]
        return old, new, log_sum

    def product(left, right):
        return lax.dot_general(
            left,
            right,
            (((0,), (0,)), ((), ())),
            precision=highest,
            preferred_element_type=f32,
        )

    turned_cross = cross.T
    right_top = jnp.broadcast_to(side[:, 1:2], (128, 128))
    right_low = jnp.broadcast_to(side[:, 2:3], (128, 128))
    final = jnp.where(lane < 64, upper[0:64, :], right_top[0:64, :])
    low = [jnp.where(iota((128, 128), 1) < 64, cross, right_low), lower]

    parts = [upper[64:128, :], turned_cross[64:128, :], right_top[64:128, :]]
    old, fresh, log_sum = panel_of(parts, 64, log_sum)
    quadratic = old[2] * fresh[2]
    first = jnp.where(lane < 64, fresh[0], fresh[2])
    change = product(old[1], jnp.concatenate([first, fresh[1]], axis=1))
    low = [low[0] - change[:, 0:128], low[1] - change[:, 128:256]]
    final = final - product(old[0][:, 0:64], first)

    parts = [low[0][0:64, :], low[1][0:64, :]]
    old, fresh, log_sum = panel_of(parts, 128, log_sum)
    quadratic = quadratic + old[0] * fresh[0]
    change = product(old[1][:, 64:128], jnp.concatenate(fresh, axis=1))
    final = final - product(old[0][:, 0:64], fresh[0])

    parts = [low[0][64:128, :] - change[:, 0:128], low[1][64:128, :] - change[:, 128:256]]
    old, fresh, log_sum = panel_of(parts, 192, log_sum)
    quadratic = quadratic + old[0] * fresh[0]
    final = final - product(old[0][:, 0:64], fresh[0])

    _, _, own = location()
    mine = jnp.where((row == own) & (col == own), coupling_ref[...], 0.0)
    self_coupling = total(mine)
    power = power_column(spectrum_ref)
    row64, col64 = iota((64, 128), 0), iota((64, 128), 1)
    block = final
    block = jnp.where(row64 == col64, block + self_coupling * power, block)
    block = jnp.where(col64 < 64, block, jnp.where(col64 == row64 + 64, 1.0, 0.0))
    tiles = [[block[8 * a : 8 * a + 8, :]] for a in range(8)]
    tiles, _, _, log_sum = eliminate_rows(tiles, 0, log_sum, board, True)
    solved = jnp.concatenate([tiles[a][0] for a in range(8)], axis=0)
    inverse = pltpu.roll(solved, 64, 1)
    top, bottom = inverse[0:32, :], inverse[32:64, :]
    row32, col32 = iota((32, 128), 0), iota((32, 128), 1)
    moved = pltpu.roll(bottom, 96, 1)
    triangle = jnp.where(col32 > row32, top, moved)
    folded = jnp.where(col32 < 32, triangle, top)
    lines = jnp.where(
        iota((16, 128), 1) < 64, folded[0:16, :], pltpu.roll(folded[16:32, :], 64, 1)
    )
    diagonal = jnp.sum(jnp.where(row32 == col32, top, 0.0), axis=0, keepdims=True)
    target = final
    target_line = jnp.concatenate([target, target], axis=0).T[64:65, :]
    final_line = jnp.where(iota((1, 128), 1) < 64, diagonal, target_line)
    whole = jnp.concatenate([lines, final_line], axis=0)
    whole = jnp.concatenate([whole] * 8, axis=0)
    for i in range(8):
        sent_ref[8 * LINES * i : 8 * LINES * (i + 1), :] = whole
    spent = jnp.sum(quadratic, axis=0, keepdims=True)
    left_over = rest[3:4, 0:1] - spent[:, 64:65]
    line = iota((8, 128), 0)
    extra_ref[...] = jnp.where(line == 0, left_over, rest[3:4, 1:2])
    logdet_ref[0] = log_sum[0, 0] / COLUMNS


def own_terms(parts, own_prior, spectrum, coupling):
    vmem = pl.BlockSpec(memory_space=pltpu.VMEM)
    smem = pl.BlockSpec(memory_space=pltpu.SMEM)
    return pl.pallas_call(
        own_kernel,
        in_specs=[vmem] * 8,
        out_specs=[vmem, vmem, smem],
        out_shape=[
            pltpu.VMEM((64 * LINES, 128), f32),
            pltpu.VMEM((8, 128), f32),
            jax.ShapeDtypeStruct((1,), f32),
        ],
        scratch_shapes=[pltpu.VMEM((32 * 14, 8, 128), f32)],
        name="own",
    )(*map(in_vmem, parts), own_prior, spectrum, in_vmem(coupling))


def three_parts(value):
    high = value.astype(jnp.bfloat16)
    rest = value - high.astype(f32)
    middle = rest.astype(jnp.bfloat16)
    low = (rest - middle.astype(f32)).astype(jnp.bfloat16)
    return high, middle, low


def gradient_kernel(
    near_ref,
    far_ref,
    coupling_ref,
    spectrum_ref,
    extra_ref,
    coeffs_ref,
    chi_ref,
    flat,
    inverse,
    target,
    weights,
    direction,
    mapped,
    answer,
    turned,
):
    for i in range(LINES):
        rows = pl.ds(i, 64, stride=LINES)
        both = jnp.concatenate([near_ref[rows, :], far_ref[rows, :]], axis=0).T
        for m in range(0, 128, 8):
            flat[pl.ds(m * LINES + i, 8, stride=LINES), :] = both[m : m + 8, :]
    line = iota((8, 128), 0)

    def straight_of(r, c):
        return flat[pl.ds((64 * (r // 16) + c) * LINES + r % 16, 8, stride=LINES), :]

    def crossed_of(c, r):
        at = (64 * (c // 16) + r) * LINES + c % 16
        return flat[at : at + 8, :]

    for r in range(32):
        corner = flat[r * LINES + 16 : r * LINES + 17, :]
        for c in range(0, 32, 8):
            if c > r:
                upper, lower = straight_of(r, c), crossed_of(c, r)
            elif c + 7 < r:
                upper, lower = crossed_of(c, r), straight_of(r, c)
            else:
                index = line + c
                straight, crossed = straight_of(r, c), crossed_of(c, r)
                upper = jnp.where(index > r, straight, crossed)
                upper = jnp.where(index == r, corner, upper)
                lower = jnp.where(index <= r, straight, crossed)
            inverse[r, c : c + 8, :] = upper
            inverse[32 + r, 32 + c : 40 + c, :] = lower
            inverse[r, 32 + c : 40 + c, :] = straight_of(r, 32 + c)
            inverse[32 + r, c : c + 8, :] = crossed_of(c, 32 + r)
    for c in range(0, 64, 8):
        target[c : c + 8, :] = flat[pl.ds((64 + c) * LINES + 16, 8, stride=LINES), :]

    row, col = iota((128, 128), 0), iota((128, 128), 1)
    mixing = jnp.where(row == col, 0.0, coupling_ref[...])
    power = power_column(spectrum_ref)
    power = jnp.broadcast_to(power, (64, 128))
    direction[...] = jnp.zeros((64, 128), f32)
    mapped[...] = jnp.zeros((64, 128), f32)
    answer[...] = jnp.zeros((64, 128), f32)
    high, middle, low = three_parts(mixing)
    weights[...] = jnp.concatenate([high, middle, high, middle, low, high], axis=0)

    def iterate(_, carry):
        inner, curved, *rows = carry
        sums = [jnp.zeros((8, 128), f32) for _ in range(8)]
        for k in range(64):
            line = sub_bcast(rows[k // 8], k % 8)
            for c in range(8):
                sums[c] = sums[c] + inverse[k, 8 * c : 8 * c + 8, :] * line
        now = jnp.concatenate(rows, axis=0)
        scaled = jnp.concatenate(sums, axis=0)
        high, middle, low = three_parts(scaled)
        wide = jnp.concatenate([high, high, middle, middle, high, low], axis=1)
        mixed = jnp.dot(wide, weights[...], preferred_element_type=f32)
        image = now + power * mixed
        old_mapped = mapped[...]
        inner_next = total(now * scaled)
        straight = total(scaled * image)
        crossing = total(scaled * old_mapped)
        ratio = inner_next / inner
        curved = straight + ratio * (2.0 * crossing + ratio * curved)
        step = inner_next / curved
        toward = scaled + ratio * direction[...]
        image = image + ratio * old_mapped
        direction[...] = toward
        mapped[...] = image
        answer[...] = answer[...] + step * toward
        now = now - step * image
        return (inner_next, curved, *[now[8 * c : 8 * c + 8, :] for c in range(8)])

    first = [target[8 * c : 8 * c + 8, :] for c in range(8)]
    lax.fori_loop(0, ITERS, iterate, (jnp.ones((1, 1), f32), jnp.zeros((1, 1), f32), *first))
    _, _, own = location()
    value = answer[...]
    gained = jnp.sum(target[...] * value, axis=0, keepdims=True)
    lane = iota((1, 128), 1)
    gained = jnp.sum(jnp.where(lane == own, gained, 0.0), axis=1, keepdims=True)
    chi = (extra_ref[0:1, 0:1] - gained) / extra_ref[1:2, 0:1]
    chi_ref[0] = chi[0, 0]
    turned[...] = jnp.concatenate([value, value], axis=0).T
    coeffs_ref[...] = turned[pl.ds(own, 1), :][:, 0:64]


def conjugate(near, far, coupling, spectrum, extra):
    vmem = pl.BlockSpec(memory_space=pltpu.VMEM)
    smem = pl.BlockSpec(memory_space=pltpu.SMEM)
    square = pltpu.VMEM((64, 128), f32)
    return pl.pallas_call(
        gradient_kernel,
        in_specs=[vmem] * 5,
        out_specs=[vmem, smem],
        out_shape=[jax.ShapeDtypeStruct((1, COMMON), f32), jax.ShapeDtypeStruct((1,), f32)],
        scratch_shapes=[
            pltpu.VMEM((WIDTH, 128), f32),
            pltpu.VMEM((64, 64, 128), f32),
            square,
            pltpu.VMEM((6 * 128, 128), jnp.bfloat16),
            square,
            square,
            square,
            pltpu.VMEM((128, 128), f32),
        ],
        name="gradient",
    )(in_vmem(near), in_vmem(far), in_vmem(coupling), spectrum, in_vmem(extra))


def body(design, noise_weight, residuals, slot_pulsar, slot_rows, own_prior, spectrum, directions):
    count = lax.axis_size("psr") * lax.axis_size("toa")
    spectrum = spectrum.reshape(1, -1)
    mine, other = gram_parts(design, noise_weight, residuals, slot_pulsar, slot_rows)
    got = lax.ppermute(other, "toa", [(u, u ^ 1) for u in range(8)])
    parts = [mine, got]
    for s in range(1, 4):
        part = mine[s] + got[s]
        parts.append(lax.ppermute(part, "toa", [(u, (u + 2 * s) % 8) for u in range(8)]))
    coupling = coupling_inverse(directions)
    sent, extra, log_dets = own_terms(parts, own_prior, spectrum, coupling)
    groups = [list(range(c, count, 2)) for c in range(2)]
    sent = sent.reshape(64, 1, WIDTH)
    near = lax.all_to_all(sent, AXES, 0, 0, tiled=True, axis_index_groups=groups)
    near = near.reshape(64 * LINES, 128)
    far = lax.ppermute(near, "toa", [(u, u ^ 1) for u in range(8)])
    coeffs, chi_square = conjugate(near, far, coupling, spectrum, extra)
    return (coeffs, log_dets, chi_square)


def solution(mesh):
    return jax.shard_map(
        body,
        mesh=mesh,
        in_specs=(
            P(AXES, None, None),
            P(AXES, None),
            P(AXES, None),
            P(AXES),
            P(AXES),
            P(AXES, None),
            P(),
            P(),
        ),
        out_specs=(P(AXES, None), P(AXES), P(AXES)),
        check_vma=False,
    )
```

```python
import jax
import jax.numpy as jnp
from jax import lax
from jax.experimental import pallas as pl
from jax.experimental.pallas import tpu as pltpu
from jax.sharding import PartitionSpec as P


GROUP_PULSARS = 8
ITERS = 8
COLUMNS = 256
COMMON = 64
STEP_BLOCKS = 8
ROWS_SENT = 264
AHEAD = True
WIDTH = 2176
LINES = WIDTH // 128
AXES = ("psr", "toa")

highest = lax.Precision.HIGHEST
f32 = jnp.float32


def location():
    toa = lax.axis_index("toa")
    return toa >> 1, toa & 1, lax.axis_index("psr") * 4 + (toa >> 1)


def in_vmem(value):
    return pltpu.with_memory_space_constraint(value, pltpu.VMEM)


def iota(shape, dim):
    return lax.broadcasted_iota(jnp.int32, shape, dim)


def sub_bcast(value, row):
    return jnp.broadcast_to(value[row : row + 1, :], value.shape)


def lane_bcast(value, lane):
    index = jnp.full(value.shape, lane, jnp.int32)
    return jnp.take_along_axis(value, index, axis=1, mode="promise_in_bounds")


def total(value):
    return jnp.sum(jnp.sum(value, axis=0, keepdims=True), axis=1, keepdims=True)


def summed_tree(parts):
    while len(parts) > 1:
        joined = [u + v for u, v in zip(parts[::2], parts[1::2])]
        parts = joined + ([parts[-1]] if len(parts) % 2 else [])
    return parts[0]


def invert_block(cols, log_sum):
    row = iota((8, 128), 0)
    for i in range(0, 8, 2):
        first, second = row == i, row == i + 1
        c0, c1 = cols[i], cols[i + 1]
        p, q = sub_bcast(c0, i), sub_bcast(c1, i)
        r, s = sub_bcast(c0, i + 1), sub_bcast(c1, i + 1)
        det = p * s - q * r
        inverse = 1.0 / det
        log_sum = log_sum + jnp.log(det)
        for k in range(8):
            if k not in (i, i + 1):
                u, v = sub_bcast(cols[k], i), sub_bcast(cols[k], i + 1)
                n0 = s * u - q * v
                n1 = p * v - r * u
                moved = cols[k] - (c0 * n0 + c1 * n1) * inverse
                moved = jnp.where(first, n0 * inverse, moved)
                cols[k] = jnp.where(second, n1 * inverse, moved)
        left = jnp.where(first, s, jnp.where(second, -r, c1 * r - c0 * s))
        right = jnp.where(first, -q, jnp.where(second, p, c0 * q - c1 * p))
        cols[i] = left * inverse
        cols[i + 1] = right * inverse
    return cols, log_sum


class Board:
    def __init__(self, ref):
        self.ref, self.used = ref, 0

    def rows(self, value):
        at = self.used
        self.used = at + 1
        self.ref[at] = value
        return [self.ref[at, k : k + 1, :] for k in range(8)]


def eliminate_rows(tiles, first_lane, log_sum, board, whole, ahead=True):
    count = len(tiles)
    width = len(tiles[0])
    before, after = [], []

    def columns(a, b):
        at = first_lane + 8 * b
        return [lane_bcast(tiles[a][at // 128], at % 128 + k) for k in range(8)]

    cols = columns(0, 0)
    for b in range(count):
        cols, log_sum = invert_block(cols, log_sum)
        last = b + 1 == count
        factors = {}
        if not last and ahead:
            factor = columns(b + 1, b)
            factors[b + 1] = factor
            coming = columns(b + 1, b + 1)
            spots = [board.rows(value) for value in factor]
            for j in range(8):
                solved = summed_tree([cols[m] * spots[m][j] for m in range(8)])
                change = summed_tree([factor[k] * sub_bcast(solved, k) for k in range(8)])
                coming[j] = coming[j] - change
        fresh, spread = [], []
        for t in range(width):
            rows = board.rows(tiles[b][t])
            fresh.append(summed_tree([cols[k] * rows[k] for k in range(8)]))
            spread.append(board.rows(fresh[t]))
        before.append(tiles[b])
        after.append(fresh)
        for a in range(0 if whole else b + 1, count):
            if a != b:
                factor = factors[a] if a in factors else columns(a, b)
                tiles[a] = [
                    tiles[a][t] - summed_tree([factor[k] * spread[t][k] for k in range(8)])
                    for t in range(width)
                ]
        if whole:
            tiles[b] = fresh
        if not last:
            cols = coming if ahead else columns(b + 1, b + 1)
    return tiles, before, after, log_sum


def gram_kernel(
    pulsar_ref,
    rows_ref,
    design_ref,
    weight_ref,
    resid_ref,
    mine_ref,
    other_ref,
    blocks,
    gram,
    fit,
    energy,
    wide_resid,
    counts,
    arrived,
):
    slots = weight_ref.shape[0]
    steps = slots // STEP_BLOCKS

    def load(step):
        where = pl.ds(step * STEP_BLOCKS, STEP_BLOCKS)
        return pltpu.make_async_copy(design_ref.at[where], blocks.at[where], arrived.at[step])

    for step in range(steps):
        load(step).start()
    gram[...] = jnp.zeros(gram.shape, f32)
    fit[...] = jnp.zeros(fit.shape, f32)
    energy[...] = jnp.zeros(energy.shape, f32)
    for k in range(GROUP_PULSARS):
        counts[k] = 0
    wide_resid[...] = resid_ref[...].astype(f32)
    lane = iota((1, 128), 1)

    def one_step(step, carry):
        load(step).wait()
        at = step * STEP_BLOCKS
        pulsars = [pulsar_ref[at + i] for i in range(STEP_BLOCKS)]
        rows = [rows_ref[at + i] for i in range(STEP_BLOCKS)]
        same = pulsars[1] == pulsars[0]
        for i in range(2, STEP_BLOCKS):
            same = same & (pulsars[i] == pulsars[0])
        low = jnp.where(same, pulsars[0], 0)
        high = jnp.where(same, pulsars[0] + 1, GROUP_PULSARS)

        def one_pulsar(pulsar, carry):
            valid = [jnp.where(pulsars[i] == pulsar, rows[i], 0) for i in range(STEP_BLOCKS)]
            number = valid[0]
            for i in range(1, STEP_BLOCKS):
                number = number + valid[i]

            @pl.when(number > 0)
            def _():
                pieces, fitted, squares = [], None, None
                for i in range(STEP_BLOCKS):
                    weight = jnp.where(lane < valid[i], weight_ref[pl.ds(at + i, 1), :], 0.0)
                    resid = wide_resid[pl.ds(at + i, 1), :]
                    turned = blocks[at + i].T.astype(f32)
                    weighted = (turned * weight).astype(jnp.bfloat16)
                    pieces.append(weighted)
                    product = weighted.astype(f32) * resid
                    square = weight * resid * resid
                    fitted = product if fitted is None else fitted + product
                    squares = square if squares is None else squares + square
                left = jnp.concatenate(pieces, axis=1)
                right = blocks[pl.ds(at, STEP_BLOCKS)].reshape(STEP_BLOCKS * 128, COLUMNS)
                gram[pulsar] = gram[pulsar] + jnp.dot(left, right, preferred_element_type=f32)
                fit[pulsar] = fit[pulsar] + fitted
                energy[pl.ds(pulsar, 1), :] = energy[pl.ds(pulsar, 1), :] + squares
                counts[pulsar] = counts[pulsar] + number

            return carry

        return lax.fori_loop(low, high, one_pulsar, carry)

    lax.fori_loop(0, steps, one_step, 0)

    row, col = iota((128, 128), 0), iota((128, 128), 1)
    line = iota((8, 128), 0)
    spot = iota((8, 128), 1)
    height, core, _ = location()

    def pack(out_ref, s, k):
        @pl.when(counts[k] == 0)
        def _():
            out_ref[s] = jnp.zeros((ROWS_SENT, 128), f32)

        @pl.when(counts[k] > 0)
        def _():
            upper = gram[k, 0:128, 0:128]
            lower = gram[k, 128:256, 128:256]
            upper = 0.5 * (upper + upper.T)
            lower = 0.5 * (lower + lower.T)
            cross = 0.5 * (gram[k, 128:256, 0:128] + gram[k, 0:128, 128:256].T)
            out_ref[s, 0:128, :] = jnp.where(col > row, upper, lower)
            out_ref[s, 128:256, :] = cross
            diagonal = jnp.sum(jnp.where(col == row, upper, 0.0), axis=0, keepdims=True)
            first = jnp.sum(fit[k, 0:128, :].T, axis=0, keepdims=True)
            second = jnp.sum(fit[k, 128:256, :].T, axis=0, keepdims=True)
            power = jnp.sum(energy[pl.ds(k, 1), :], axis=1, keepdims=True)
            number = counts[k].astype(f32)
            last = jnp.where(spot == 0, power, jnp.where(spot == 1, number, 0.0))
            rest = jnp.where(line == 3, last, 0.0)
            rest = jnp.where(line == 0, diagonal, rest)
            rest = jnp.where(line == 1, first, rest)
            out_ref[s, 256:264, :] = jnp.where(line == 2, second, rest)

    for s in range(4):
        base = 2 * ((height + s) & 3)
        pack(other_ref, s, base + 1 - core)
        pack(mine_ref, s, base + core)


def gram_parts(design, weight, residuals, slot_pulsar, slot_rows):
    slots = design.shape[0]
    piece = pltpu.VMEM((4, ROWS_SENT, 128), f32)
    smem = pl.BlockSpec(memory_space=pltpu.SMEM)
    vmem = pl.BlockSpec(memory_space=pltpu.VMEM)
    hbm = pl.BlockSpec(memory_space=pl.ANY)
    return pl.pallas_call(
        gram_kernel,
        in_specs=[smem, smem, hbm, vmem, vmem],
        out_specs=[vmem, vmem],
        scratch_shapes=[
            pltpu.VMEM((slots, 128, COLUMNS), jnp.bfloat16),
            pltpu.VMEM((GROUP_PULSARS, COLUMNS, COLUMNS), f32),
            pltpu.VMEM((GROUP_PULSARS, COLUMNS, 128), f32),
            pltpu.VMEM((GROUP_PULSARS, 128), f32),
            pltpu.VMEM((slots, 128), f32),
            pltpu.SMEM((GROUP_PULSARS,), jnp.int32),
            pltpu.SemaphoreType.DMA((slots // STEP_BLOCKS,)),
        ],
        out_shape=[piece, piece],
        name="gram",
    )(slot_pulsar, slot_rows, design, weight, residuals)


def coupling_kernel(directions_ref, out_ref, board_ref):
    _, core, _ = location()
    row, col = iota((128, 128), 0), iota((128, 128), 1)
    source = jnp.where(col < 64, 2 * col + core, 2 * col - 127 - core)
    chosen = (row == source).astype(f32)
    lines = jnp.concatenate([directions_ref[...], jnp.zeros((5, 128), f32)], axis=0)
    lines = jnp.dot(lines, chosen, precision=highest, preferred_element_type=f32)
    turned = lines.T
    cosines = jnp.zeros((128, 128), f32)
    for i in range(3):
        cosines = cosines + turned[:, i : i + 1] * lines[i : i + 1, :]
    cosines = jnp.clip(cosines, -1.0, 1.0)
    same = row == col
    spread = jnp.where(same, 1.0, 0.5 * (1.0 - cosines))
    curve = 1.5 * spread * jnp.log(spread) - 0.25 * spread + 0.5
    correlation = jnp.where(same, 1.0, curve)
    identity = jnp.where(same, 1.0, 0.0)
    tiles = [
        [correlation[8 * a : 8 * a + 8, :], identity[8 * a : 8 * a + 8, :]] for a in range(16)
    ]
    board = Board(board_ref)
    tiles, _, _, _ = eliminate_rows(tiles, 0, jnp.zeros((8, 128), f32), board, True, AHEAD)
    for a in range(16):
        out_ref[8 * a : 8 * a + 8, :] = tiles[a][1]


def coupling_inverse(directions):
    return pl.pallas_call(
        coupling_kernel,
        in_specs=[pl.BlockSpec(memory_space=pltpu.VMEM)],
        out_specs=pl.BlockSpec(memory_space=pltpu.VMEM),
        out_shape=pltpu.VMEM((128, 128), f32),
        scratch_shapes=[pltpu.VMEM((16 * 12, 8, 128), f32)],
        name="coupling",
    )(directions)


def power_column(spectrum_ref):
    inverse = 1.0 / spectrum_ref[...]
    half = iota((64, 32), 0) >> 1
    spread = jnp.where(iota((64, 32), 1) == half, jnp.broadcast_to(inverse, (64, 32)), 0.0)
    return jnp.sum(spread, axis=1, keepdims=True)


def own_kernel(
    kept,
    part0,
    part1,
    part2,
    part3,
    prior_ref,
    spectrum_ref,
    coupling_ref,
    sent_ref,
    extra_ref,
    logdet_ref,
    board_ref,
):
    row, col = iota((128, 128), 0), iota((128, 128), 1)

    def summed(lo, hi):
        near = kept[0, lo:hi, :] + part0[0, lo:hi, :]
        return (near + part1[lo:hi, :]) + (part2[lo:hi, :] + part3[lo:hi, :])

    packed = summed(0, 128)
    cross = summed(128, 256)
    rest = summed(256, 264)
    turned = packed.T
    prior = 1.0 / prior_ref[...]
    prior = jnp.concatenate([jnp.zeros((1, 64), f32), prior], axis=1)
    upper = jnp.where(col > row, packed, turned)
    upper = jnp.where(col == row, rest[0:1, :] + prior[:, 0:128], upper)
    lower = jnp.where(col <= row, packed, turned)
    lower = jnp.where(col == row, lower + prior[:, 128:256], lower)
    side = rest.T
    lane = iota((64, 128), 1)
    log_sum = jnp.zeros((8, 128), f32)

    board = Board(board_ref)

    def panel_of(parts, at, log_sum):
        tiles = [[part[8 * a : 8 * a + 8, :] for part in parts] for a in range(8)]
        _, before, after, log_sum = eliminate_rows(tiles, at, log_sum, board, False)
        old, new = [
            [jnp.concatenate([rows[a][t] for a in range(8)], axis=0) for t in range(len(parts))]
            for rows in (before, after)
        ]
        return old, new, log_sum

    def product(left, right):
        return lax.dot_general(
            left,
            right,
            (((0,), (0,)), ((), ())),
            precision=highest,
            preferred_element_type=f32,
        )

    turned_cross = cross.T
    right_top = jnp.broadcast_to(side[:, 1:2], (128, 128))
    right_low = jnp.broadcast_to(side[:, 2:3], (128, 128))
    final = jnp.where(lane < 64, upper[0:64, :], right_top[0:64, :])
    low = [jnp.where(iota((128, 128), 1) < 64, cross, right_low), lower]

    parts = [upper[64:128, :], turned_cross[64:128, :], right_top[64:128, :]]
    old, fresh, log_sum = panel_of(parts, 64, log_sum)
    quadratic = old[2] * fresh[2]
    first = jnp.where(lane < 64, fresh[0], fresh[2])
    change = product(old[1], jnp.concatenate([first, fresh[1]], axis=1))
    low = [low[0] - change[:, 0:128], low[1] - change[:, 128:256]]
    final = final - product(old[0][:, 0:64], first)

    parts = [low[0][0:64, :], low[1][0:64, :]]
    old, fresh, log_sum = panel_of(parts, 128, log_sum)
    quadratic = quadratic + old[0] * fresh[0]
    change = product(old[1][:, 64:128], jnp.concatenate(fresh, axis=1))
    final = final - product(old[0][:, 0:64], fresh[0])

    parts = [low[0][64:128, :] - change[:, 0:128], low[1][64:128, :] - change[:, 128:256]]
    old, fresh, log_sum = panel_of(parts, 192, log_sum)
    quadratic = quadratic + old[0] * fresh[0]
    final = final - product(old[0][:, 0:64], fresh[0])

    _, _, own = location()
    mine = jnp.where((row == own) & (col == own), coupling_ref[...], 0.0)
    self_coupling = total(mine)
    power = power_column(spectrum_ref)
    row64, col64 = iota((64, 128), 0), iota((64, 128), 1)
    block = final
    block = jnp.where(row64 == col64, block + self_coupling * power, block)
    block = jnp.where(col64 < 64, block, jnp.where(col64 == row64 + 64, 1.0, 0.0))
    tiles = [[block[8 * a : 8 * a + 8, :]] for a in range(8)]
    tiles, _, _, log_sum = eliminate_rows(tiles, 0, log_sum, board, True)
    solved = jnp.concatenate([tiles[a][0] for a in range(8)], axis=0)
    inverse = pltpu.roll(solved, 64, 1)
    top, bottom = inverse[0:32, :], inverse[32:64, :]
    row32, col32 = iota((32, 128), 0), iota((32, 128), 1)
    moved = pltpu.roll(bottom, 96, 1)
    triangle = jnp.where(col32 > row32, top, moved)
    folded = jnp.where(col32 < 32, triangle, top)
    lines = jnp.where(
        iota((16, 128), 1) < 64, folded[0:16, :], pltpu.roll(folded[16:32, :], 64, 1)
    )
    diagonal = jnp.sum(jnp.where(row32 == col32, top, 0.0), axis=0, keepdims=True)
    target = final
    target_line = jnp.concatenate([target, target], axis=0).T[64:65, :]
    final_line = jnp.where(iota((1, 128), 1) < 64, diagonal, target_line)
    whole = jnp.concatenate([lines, final_line], axis=0)
    whole = jnp.concatenate([whole] * 8, axis=0)
    for i in range(8):
        sent_ref[8 * LINES * i : 8 * LINES * (i + 1), :] = whole
    spent = jnp.sum(quadratic, axis=0, keepdims=True)
    left_over = rest[3:4, 0:1] - spent[:, 64:65]
    line = iota((8, 128), 0)
    extra_ref[...] = jnp.where(line == 0, left_over, rest[3:4, 1:2])
    logdet_ref[0] = log_sum[0, 0] / COLUMNS


def own_terms(parts, own_prior, spectrum, coupling):
    vmem = pl.BlockSpec(memory_space=pltpu.VMEM)
    smem = pl.BlockSpec(memory_space=pltpu.SMEM)
    return pl.pallas_call(
        own_kernel,
        in_specs=[vmem] * 8,
        out_specs=[vmem, vmem, smem],
        out_shape=[
            pltpu.VMEM((64 * LINES, 128), f32),
            pltpu.VMEM((8, 128), f32),
            jax.ShapeDtypeStruct((1,), f32),
        ],
        scratch_shapes=[pltpu.VMEM((32 * 14, 8, 128), f32)],
        name="own",
    )(*map(in_vmem, parts), own_prior, spectrum, in_vmem(coupling))


def three_parts(value):
    high = value.astype(jnp.bfloat16)
    rest = value - high.astype(f32)
    middle = rest.astype(jnp.bfloat16)
    low = (rest - middle.astype(f32)).astype(jnp.bfloat16)
    return high, middle, low


def gradient_kernel(
    near_ref,
    far_ref,
    coupling_ref,
    spectrum_ref,
    extra_ref,
    coeffs_ref,
    chi_ref,
    flat,
    inverse,
    target,
    weights,
    resid,
    scale,
    direction,
    mapped,
    solved,
    twice,
    answer,
    turned,
):
    for i in range(LINES):
        rows = pl.ds(i, 64, stride=LINES)
        both = jnp.concatenate([near_ref[rows, :], far_ref[rows, :]], axis=0).T
        for m in range(0, 128, 8):
            flat[pl.ds(m * LINES + i, 8, stride=LINES), :] = both[m : m + 8, :]
    line = iota((8, 128), 0)

    def straight_of(r, c):
        return flat[pl.ds((64 * (r // 16) + c) * LINES + r % 16, 8, stride=LINES), :]

    def crossed_of(c, r):
        at = (64 * (c // 16) + r) * LINES + c % 16
        return flat[at : at + 8, :]

    for r in range(32):
        corner = flat[r * LINES + 16 : r * LINES + 17, :]
        for c in range(0, 32, 8):
            if c > r:
                upper, lower = straight_of(r, c), crossed_of(c, r)
            elif c + 7 < r:
                upper, lower = crossed_of(c, r), straight_of(r, c)
            else:
                index = line + c
                straight, crossed = straight_of(r, c), crossed_of(c, r)
                upper = jnp.where(index > r, straight, crossed)
                upper = jnp.where(index == r, corner, upper)
                lower = jnp.where(index <= r, straight, crossed)
            inverse[r, c : c + 8, :] = upper
            inverse[32 + r, 32 + c : 40 + c, :] = lower
            inverse[r, 32 + c : 40 + c, :] = straight_of(r, 32 + c)
            inverse[32 + r, c : c + 8, :] = crossed_of(c, 32 + r)
    for c in range(0, 64, 8):
        target[c : c + 8, :] = flat[pl.ds((64 + c) * LINES + 16, 8, stride=LINES), :]

    row, col = iota((128, 128), 0), iota((128, 128), 1)
    mixing = jnp.where(row == col, 0.0, coupling_ref[...])
    power = power_column(spectrum_ref)
    power = jnp.broadcast_to(power, (64, 128))
    zero = jnp.zeros((64, 128), f32)
    for ref in (direction, mapped, solved, twice, answer):
        ref[...] = zero
    high, middle, low = three_parts(mixing)
    weights[...] = jnp.concatenate([high, middle, high, middle, low, high], axis=0)

    def applied(rows):
        sums = [jnp.zeros((8, 128), f32) for _ in range(8)]
        for k in range(64):
            line = sub_bcast(rows[k // 8], k % 8)
            for c in range(8):
                sums[c] = sums[c] + inverse[k, 8 * c : 8 * c + 8, :] * line
        scaled = jnp.concatenate(sums, axis=0)
        high, middle, low = three_parts(scaled)
        wide = jnp.concatenate([high, high, middle, middle, high, low], axis=1)
        mixed = jnp.dot(wide, weights[...], preferred_element_type=f32)
        return scaled, jnp.concatenate(rows, axis=0) + power * mixed

    def in_rows(value):
        return [value[8 * c : 8 * c + 8, :] for c in range(8)]

    def scalars(inner, curved, now, scaled, image):
        inner_next = total(now * scaled)
        straight = total(scaled * image)
        crossing = total(scaled * mapped[...])
        ratio = inner_next / inner
        curved = straight + ratio * (2.0 * crossing + ratio * curved)
        return inner_next, curved, ratio, inner_next / curved

    resid[...] = target[...]
    first, image = applied(in_rows(target[...]))
    scale[...] = first

    def iterate(_, carry):
        inner, curved, *rows = carry
        image = jnp.concatenate(rows, axis=0)
        now, scaled = resid[...], scale[...]
        inner, curved, ratio, step = scalars(inner, curved, now, scaled, image)
        solved_image, next_image = applied(rows)
        toward = scaled + ratio * direction[...]
        along = image + ratio * mapped[...]
        solved_now = solved_image + ratio * solved[...]
        twice_now = next_image + ratio * twice[...]
        direction[...] = toward
        mapped[...] = along
        solved[...] = solved_now
        twice[...] = twice_now
        answer[...] = answer[...] + step * toward
        resid[...] = now - step * along
        scale[...] = scaled - step * solved_now
        return (inner, curved, *in_rows(image - step * twice_now))

    start = (jnp.ones((1, 1), f32), jnp.zeros((1, 1), f32), *in_rows(image))
    inner, curved, *rows = lax.fori_loop(0, ITERS - 1, iterate, start)
    image = jnp.concatenate(rows, axis=0)
    inner, curved, ratio, step = scalars(inner, curved, resid[...], scale[...], image)
    answer[...] = answer[...] + step * (scale[...] + ratio * direction[...])
    _, _, own = location()
    value = answer[...]
    gained = jnp.sum(target[...] * value, axis=0, keepdims=True)
    lane = iota((1, 128), 1)
    gained = jnp.sum(jnp.where(lane == own, gained, 0.0), axis=1, keepdims=True)
    chi = (extra_ref[0:1, 0:1] - gained) / extra_ref[1:2, 0:1]
    chi_ref[0] = chi[0, 0]
    turned[...] = jnp.concatenate([value, value], axis=0).T
    coeffs_ref[...] = turned[pl.ds(own, 1), :][:, 0:64]


def conjugate(near, far, coupling, spectrum, extra):
    vmem = pl.BlockSpec(memory_space=pltpu.VMEM)
    smem = pl.BlockSpec(memory_space=pltpu.SMEM)
    square = pltpu.VMEM((64, 128), f32)
    return pl.pallas_call(
        gradient_kernel,
        in_specs=[vmem] * 5,
        out_specs=[vmem, smem],
        out_shape=[jax.ShapeDtypeStruct((1, COMMON), f32), jax.ShapeDtypeStruct((1,), f32)],
        scratch_shapes=[
            pltpu.VMEM((WIDTH, 128), f32),
            pltpu.VMEM((64, 64, 128), f32),
            square,
            pltpu.VMEM((6 * 128, 128), jnp.bfloat16),
            *[square] * 7,
            pltpu.VMEM((128, 128), f32),
        ],
        name="gradient",
    )(in_vmem(near), in_vmem(far), in_vmem(coupling), spectrum, in_vmem(extra))


def body(design, noise_weight, residuals, slot_pulsar, slot_rows, own_prior, spectrum, directions):
    count = lax.axis_size("psr") * lax.axis_size("toa")
    spectrum = spectrum.reshape(1, -1)
    mine, other = gram_parts(design, noise_weight, residuals, slot_pulsar, slot_rows)
    got = lax.ppermute(other, "toa", [(u, u ^ 1) for u in range(8)])
    parts = [mine, got]
    for s in range(1, 4):
        part = mine[s] + got[s]
        parts.append(lax.ppermute(part, "toa", [(u, (u + 2 * s) % 8) for u in range(8)]))
    coupling = coupling_inverse(directions)
    sent, extra, log_dets = own_terms(parts, own_prior, spectrum, coupling)
    groups = [list(range(c, count, 2)) for c in range(2)]
    sent = sent.reshape(64, 1, WIDTH)
    near = lax.all_to_all(sent, AXES, 0, 0, tiled=True, axis_index_groups=groups)
    near = near.reshape(64 * LINES, 128)
    far = lax.ppermute(near, "toa", [(u, u ^ 1) for u in range(8)])
    coeffs, chi_square = conjugate(near, far, coupling, spectrum, extra)
    return (coeffs, log_dets, chi_square)


def solution(mesh):
    return jax.shard_map(
        body,
        mesh=mesh,
        in_specs=(
            P(AXES, None, None),
            P(AXES, None),
            P(AXES, None),
            P(AXES),
            P(AXES),
            P(AXES, None),
            P(),
            P(),
        ),
        out_specs=(P(AXES, None), P(AXES), P(AXES)),
        check_vma=False,
    )
```
